32 devices in a mesh: wide: 8 (over z, x), narrow: 4 (over y, core).
Axes of the slice: x: 2, y: 2, z: 4, core: 2. Of those that a mesh axis runs over, the one named last changes fastest.
Arguments:
- tokens_in: bfloat16 [2048, 2048], P('wide'), may hold values from -7 to 7
- seg_ids: int32 [2048], P('wide'), may hold values from 0 to 7, as said below
- routes: int32 [2048, 6], P('wide'), may hold values from 0 to 15, all different within a row; in each aligned block of 256 rows (0 to 255, 256 to 511, ...) at most 144 rows name the same one
- gate_vals: float32 [2048, 6], P('wide'), may hold values from 0.1 to 0.6
- attn_gain: float32 [2048], replicated, may hold values from 0.5 to 1.5
- w_query: bfloat16 [2048, 3072], P('wide', 'narrow')
- w_latent: bfloat16 [2048, 576], P('wide')
- latent_gain: float32 [512], replicated, may hold values from 0.5 to 1.5
- w_expand: bfloat16 [512, 4096], P('wide', 'narrow'), may hold values from -0.25 to 0.25
- w_output: bfloat16 [2048, 2048], P('narrow', 'wide'), may hold values from -0.375 to 0.375
- ffn_gain: float32 [2048], replicated, may hold values from 0.5 to 1.5
- w_shared_in: bfloat16 [2048, 2, 2816], P('wide', None, 'narrow'), may hold values from -0.125 to 0.125
- w_shared_out: bfloat16 [2816, 2048], P('narrow', 'wide'), may hold values from -0.21875 to 0.21875
- w_expert_in: bfloat16 [16, 2048, 2, 1408], P('wide', None, None, 'narrow'), may hold values from -0.125 to 0.125
- w_expert_out: bfloat16 [16, 1408, 2048], P('wide', 'narrow'), may hold values from -0.3125 to 0.3125
- grad_output: bfloat16 [2048, 2048], P('wide'), may hold values from -6 to 6
Outputs:
- layer_out: bfloat16 [2048, 2048], P('wide', 'narrow')
- grad_tokens: float32 [2048, 2048], P('wide')
- grad_attn_gain: float32 [2048], P('wide')
- grad_w_query: float32 [2048, 3072], P('wide', 'narrow')
- grad_w_latent: float32 [2048, 576], P('wide')
- grad_latent_gain: float32 [512], P('wide')
- grad_w_expand: float32 [512, 4096], P('wide', 'narrow')
- grad_w_output: float32 [2048, 2048], P('narrow', 'wide')
- grad_ffn_gain: float32 [2048], P('wide')
- grad_shared_in: float32 [2048, 2, 2816], P('wide', None, 'narrow')
- grad_shared_out: float32 [2816, 2048], P('narrow', 'wide')
- grad_expert_in: float32 [16, 2048, 2, 1408], P('wide', None, None, 'narrow')
- grad_expert_out: float32 [16, 1408, 2048], P('wide', 'narrow')
The draws below stay inside these ranges and needn't reach their ends.
Inputs may be any that keep to these rules, and one draw needn't show every extreme that they name: `seg_ids`: ids never decrease within one device's block of tokens; equal ids there mark one sequence, which lies inside that block; a block holds one to eight sequences, and some block holds a single sequence filling it. `routes`: each row names 6 different experts; within the 256 rows of one device no expert is named more than 144 times, and in some device's rows one expert is named exactly 144 times.
All inputs are finite; a program needn't handle non-finite values.
Results may differ from the reference program's by a relative error of at most 0.015.
Values may be sent and summed in bfloat16 or wider, within the bound.
A program may use at most 320 MiB of HBM per device.

```python
import math
import jax
import jax.numpy as jnp
import numpy as np
from jax import lax

D = 2048
H = 16
DH = 128
DR = 64
KVR = 512
FF = 1408
TOP = 6
TOK_DEV = 256
SFF = 2816
EXPERTS = 16
TOKENS = 2048
CAP = 144
N_WIDE = 8


def draw_seg_ids(key, part):
    key_cuts, key_counts, key_order = jax.random.split(key, 3)
    block_count = TOKENS // TOK_DEV
    cut_points = jax.random.randint(key_cuts, (block_count, 7), 1, TOK_DEV)
    active_counts = jax.random.randint(key_counts, (block_count,), 0, 8)
    block_order = jax.random.permutation(key_order, block_count)
    active_counts = jnp.where(block_order == 0, 0, jnp.where(block_order == 1, 7, active_counts))
    active = jnp.arange(7)[None, :] < active_counts[:, None]
    cut_points = jnp.where(active, cut_points, TOK_DEV)
    places = jnp.arange(TOK_DEV)
    seg_local = jnp.sum((places[None, :, None] >= cut_points[:, None, :]).astype(jnp.int32), axis=2)
    return seg_local.reshape(-1).astype(jnp.int32)


def draw_tokens_in(key, part):
    key_base = jax.random.fold_in(jax.random.fold_in(key, 11), 0)
    base_rows = jnp.clip(jax.random.normal(key_base, (TOKENS, D), jnp.float32), -6.0, 6.0)
    return base_rows.astype(jnp.bfloat16)


def attention_inputs(key):
    key_query, key_latent = jax.random.split(jax.random.fold_in(key, 21), 2)
    scale_in = D ** (-0.5)
    latent_w = jnp.clip(jax.random.normal(key_latent, (D, KVR + DR), jnp.float32), -6.0, 6.0) * scale_in
    query_w = jnp.clip(jax.random.normal(key_query, (D, H, DH + DR), jnp.float32), -6.0, 6.0) * scale_in
    return (query_w.reshape(D, H * (DH + DR)), latent_w)


def draw_w_query(key, part):
    query_w, latent_w = attention_inputs(key)
    return query_w.astype(jnp.bfloat16)


def draw_w_latent(key, part):
    query_w, latent_w = attention_inputs(key)
    return latent_w.astype(jnp.bfloat16)


def block_scale(own_key, dims, pieces, least, top_value):
    loudness = 1.0
    for axis_at, blocks in pieces:
        draws = jax.random.uniform(jax.random.fold_in(jax.random.fold_in(own_key, 6), axis_at), (blocks,), jnp.float32, least / len(pieces), top_value / len(pieces))
        loudness = loudness * jnp.repeat(jnp.exp(draws), dims[axis_at] // blocks).reshape((-1,) + (1,) * (len(dims) - 1 - axis_at))
    return loudness


def assign_block(key, own, number, rows, amount, top, most, skew):
    sequence = jax.random.permutation(key, amount)
    packed, ordinary = load_shares(amount, rows * top, most, skew, True), load_shares(amount, rows * top, most, skew, False)
    places = jnp.arange(amount)

    def named(sizes, offset_by):
        used = int((sizes > 0).sum())
        fixed = max(1, used // 4)
        moved = fixed + (places - fixed + offset_by * (used - fixed)) % max(1, amount - fixed)
        return jnp.zeros((amount,), jnp.int32).at[sequence[jnp.where(places < fixed, places, moved)]].set(jnp.asarray(sizes, jnp.int32))

    sizes = jnp.where(number % 4 == 0, named(packed, number // 4), named(ordinary, number - number // 4 - 1))
    mixed = jax.random.permutation(jax.random.fold_in(own, 3), amount)
    source_of, sink = mixed[0:amount // 2 * 2:2], mixed[1:amount // 2 * 2:2]
    room = jnp.minimum(sizes[source_of] - 1, most - sizes[sink]) // 2
    room = jnp.where((source_of == sequence[0]) | (sink == sequence[0]) | (sizes[sink] == 0), 0, jnp.maximum(room, 0))
    moved = jax.random.randint(jax.random.fold_in(own, 4), (amount // 2,), 0, 1 << 20) % (room + 1)
    sizes = sizes.at[source_of].add(-moved).at[sink].add(moved)
    labels = jnp.searchsorted(jnp.cumsum(sizes), jnp.arange(rows * top), side="right").astype(jnp.int32)
    table = labels.reshape(top, rows).T
    table = table[jax.random.permutation(jax.random.fold_in(own, 1), rows)]
    offset_by = jax.random.randint(jax.random.fold_in(own, 2), (rows, 1), 0, top)
    return jnp.take_along_axis(table, (jnp.arange(top)[None, :] + offset_by) % top, axis=1)


def load_shares(amount, total, reach, lean, full):
    weights = [(1 << 20) // math.isqrt(grade ** lean) + 1 for grade in range(1, amount + 1)]
    largest = reach if full else min(reach, max(-(-total // amount), total * weights[0] // sum(weights)))
    least = 1 if total - largest >= amount - 1 else 0
    holding, surplus = [largest] + [least] * (amount - 1), total - largest - least * (amount - 1)
    while surplus > 0:
        free = [i for i in range(1, amount) if holding[i] < largest] or [i for i in range(1, amount) if holding[i] < reach]
        whole, left = sum([weights[i] for i in free]), surplus
        for i in free:
            more = min(reach - holding[i], max(1, left * weights[i] // whole), surplus)
            holding[i] = holding[i] + more
            surplus = surplus - more
    return np.array(holding)


def normal_values(key, shape, width, reach, cuts=(), held_as=jnp.bfloat16):
    loudness = block_scale(key, shape, cuts, -0.22, 0.18) if cuts else 1.0
    result = jax.random.normal(key, shape, jnp.float32) * width * loudness
    return jnp.minimum(jnp.maximum(result, -reach), reach).astype(held_as)


def setup_inputs(seed: int = 0) -> dict:
    splits = jax.random.split(jax.random.key(seed), 17)
    tokens_in = draw_tokens_in(jax.random.fold_in(splits[16], 71), 0)
    seg_ids = draw_seg_ids(jax.random.fold_in(splits[16], 71), 0)
    routes_keys = jax.random.split(jax.random.fold_in(splits[2], 1), TOKENS // TOK_DEV)
    routes_turns = jax.random.permutation(jax.random.fold_in(splits[2], 3), TOKENS // TOK_DEV)
    routes = jax.vmap(lambda own, number: assign_block(jax.random.fold_in(splits[2], 2), own, number, TOK_DEV, EXPERTS, TOP, CAP, 1))(routes_keys, routes_turns).reshape((TOKENS, TOP))
    gate_vals = jnp.clip(0.1 + 0.5 * jax.random.uniform(splits[3], (TOKENS, TOP), jnp.float32) ** block_scale(splits[3], (TOKENS, TOP), ((0, 8),), -0.2, 0.2), 0.1, 0.6)
    attn_gain = jnp.clip(1.0 + 0.1 * jax.random.normal(splits[4], (D,), jnp.float32), 0.5, 1.5)
    w_query = draw_w_query(jax.random.fold_in(splits[16], 71), 0)
    w_latent = draw_w_latent(jax.random.fold_in(splits[16], 71), 0)
    latent_gain = jnp.clip(1.0 + 0.1 * jax.random.normal(splits[7], (KVR,), jnp.float32), 0.5, 1.5)
    w_expand = normal_values(splits[8], (KVR, 2 * H * DH), KVR ** -0.5, 0.25, ((0, 8), (1, 4)))
    w_output = normal_values(splits[9], (H * DH, D), (H * DH // 8) ** -0.5, 0.375, ((0, 4), (1, 8)))
    ffn_gain = jnp.clip(1.0 + 0.1 * jax.random.normal(splits[10], (D,), jnp.float32), 0.5, 1.5)
    w_shared_in = normal_values(splits[11], (D, 2, SFF), D ** -0.5, 0.125, ((0, 8), (2, 4)))
    w_shared_out = normal_values(splits[12], (SFF, D), (SFF // 4) ** -0.5, 0.21875, ((0, 4), (1, 8)))
    w_expert_in = normal_values(splits[13], (EXPERTS, D, 2, FF), D ** -0.5, 0.125, ((0, 8), (3, 4)))
    w_expert_out = normal_values(splits[14], (EXPERTS, FF, D), (FF // 4) ** -0.5, 0.3125, ((0, 8), (1, 4)))
    grad_output = normal_values(splits[15], (TOKENS, D), 1.0, 6.0, ((0, 8),))
    return {"tokens_in": tokens_in, "seg_ids": seg_ids, "routes": routes, "gate_vals": gate_vals, "attn_gain": attn_gain, "w_query": w_query, "w_latent": w_latent, "latent_gain": latent_gain, "w_expand": w_expand, "w_output": w_output, "ffn_gain": ffn_gain, "w_shared_in": w_shared_in, "w_shared_out": w_shared_out, "w_expert_in": w_expert_in, "w_expert_out": w_expert_out, "grad_output": grad_output}


EPS = 1e-06
THETA = 50000.0
NEG_BIG = -1e+30

def positions(seg_ids):
    row_index = jnp.arange(seg_ids.shape[0], dtype=jnp.int32)
    starts = jnp.concatenate([jnp.ones((1,), dtype=bool), seg_ids[1:] != seg_ids[:-1]])
    begins = lax.cummax(jnp.where(starts, row_index, 0), axis=0)
    return (row_index - begins).astype(jnp.float32)

def rotary_tables(pos_float):
    half_dim = DR // 2
    inv_freq = THETA ** (-(jnp.arange(half_dim, dtype=jnp.float32) * 2.0 / DR))
    angles = pos_float[:, None] * inv_freq[None, :]
    return (jnp.cos(angles), jnp.sin(angles))

def rotate(values, cos_tab, sin_tab):
    half_dim = values.shape[-1] // 2
    lower_half = values[..., :half_dim]
    upper_half = values[..., half_dim:]
    return jnp.concatenate([lower_half * cos_tab - upper_half * sin_tab, upper_half * cos_tab + lower_half * sin_tab], -1)

def unrotate(values, cos_tab, sin_tab):
    half_dim = values.shape[-1] // 2
    lower_half = values[..., :half_dim]
    upper_half = values[..., half_dim:]
    return jnp.concatenate([lower_half * cos_tab + upper_half * sin_tab, upper_half * cos_tab - lower_half * sin_tab], -1)

def rms_forward(values, gain_vec):
    inv_rms = lax.rsqrt(lax.optimization_barrier(jnp.mean(values * values, axis=-1, keepdims=True)) + EPS)
    return (values * inv_rms * gain_vec, inv_rms)

def rms_backward(values, inv_rms, gain_vec, grad_out):
    scaled = grad_out * gain_vec
    grad_in = inv_rms * scaled - values * inv_rms ** 3 * lax.optimization_barrier(jnp.mean(values * scaled, axis=-1, keepdims=True))
    grad_gain = lax.optimization_barrier(jnp.sum(grad_out * values * inv_rms, axis=0))
    return (grad_in, grad_gain)

def swiglu(gate_up):
    gate_part = gate_up[..., 0, :]
    up_part = gate_up[..., 1, :]
    return gate_part * jax.nn.sigmoid(gate_part) * up_part

def swiglu_grad(gate_up, grad_act):
    gate_part = gate_up[..., 0, :]
    up_part = gate_up[..., 1, :]
    sigmoid_val = jax.nn.sigmoid(gate_part)
    grad_gate = grad_act * up_part * sigmoid_val * (1.0 + gate_part * (1.0 - sigmoid_val))
    grad_up = grad_act * gate_part * sigmoid_val
    return jnp.stack([grad_gate, grad_up], axis=-2)

def masked_scores(q_heads, k_heads, seg_rows, seg_cols, row_pos, col_pos):
    scale = (DH + DR) ** (-0.5)
    scores = jnp.einsum('hqc,hkc->hqk', q_heads.astype(jnp.float32), k_heads.astype(jnp.float32)) * scale
    allowed = (seg_rows[:, None] == seg_cols[None, :]) & (col_pos[None, :] <= row_pos[:, None])
    return jnp.where(allowed[None], scores, NEG_BIG)

def attend_forward(q_heads, k_heads, v_heads, seg_rows, seg_cols, row_pos, col_pos):
    scores = masked_scores(q_heads, k_heads, seg_rows, seg_cols, row_pos, col_pos)
    top_score = lax.optimization_barrier(jnp.max(scores, axis=-1, keepdims=True))
    log_total = top_score + jnp.log(lax.optimization_barrier(jnp.sum(jnp.exp(scores - top_score), axis=-1, keepdims=True)))
    prob_low = jnp.exp(scores - log_total).astype(jnp.bfloat16)
    attended = jnp.einsum('hqk,hkd->hqd', prob_low.astype(jnp.float32), v_heads.astype(jnp.float32))
    return (attended.astype(jnp.bfloat16), log_total)

def attend_backward(q_heads, k_heads, v_heads, grad_att, log_total, seg_rows, seg_cols, row_pos, col_pos):
    scale = (DH + DR) ** (-0.5)
    scores = masked_scores(q_heads, k_heads, seg_rows, seg_cols, row_pos, col_pos)
    prob_full = jnp.exp(scores - log_total)
    prob_low = prob_full.astype(jnp.bfloat16)
    grad_v = jnp.einsum('hqk,hqd->hkd', prob_low.astype(jnp.float32), grad_att.astype(jnp.float32))
    grad_prob = jnp.einsum('hqd,hkd->hqk', grad_att.astype(jnp.float32), v_heads.astype(jnp.float32))
    row_dot = lax.optimization_barrier(jnp.sum(prob_full * grad_prob, axis=-1, keepdims=True))
    grad_scores = (prob_full * (grad_prob - row_dot) * scale).astype(jnp.bfloat16)
    grad_q = jnp.einsum('hqk,hkc->hqc', grad_scores.astype(jnp.float32), k_heads.astype(jnp.float32))
    grad_k = jnp.einsum('hqk,hqc->hkc', grad_scores.astype(jnp.float32), q_heads.astype(jnp.float32))
    return (grad_q, grad_k, grad_v)

def slot_layout(route_blk, gate_blk, num_experts, capacity):
    tok_count = route_blk.shape[0]
    top_count = route_blk.shape[1]
    flat_routes = route_blk.reshape(-1)
    onehot = (flat_routes[:, None] == jnp.arange(num_experts, dtype=jnp.int32)[None, :]).astype(jnp.int32)
    earlier = jnp.cumsum(onehot, axis=0) - onehot
    slot_rank = lax.optimization_barrier(jnp.sum(earlier * onehot, axis=1))
    slot_ids = (flat_routes * capacity + slot_rank).astype(jnp.int32)
    token_ids = (jnp.arange(tok_count * top_count, dtype=jnp.int32) // top_count).astype(jnp.int32)
    slot_tokens = jnp.full((num_experts * capacity,), tok_count, jnp.int32).at[slot_ids].set(token_ids)
    slot_gates = jnp.zeros((num_experts * capacity,), jnp.float32).at[slot_ids].set(gate_blk.reshape(-1))
    return (slot_ids, slot_tokens, slot_gates)

def expert_tables(routes, gate_vals):
    route_blocks = routes.reshape(N_WIDE, TOK_DEV, TOP)
    gate_blocks = gate_vals.reshape(N_WIDE, TOK_DEV, TOP)

    def one_block(route_blk, gate_blk):
        return slot_layout(route_blk, gate_blk, EXPERTS, CAP)
    slot_ids, slot_tokens, slot_gates = jax.vmap(one_block)(route_blocks, gate_blocks)
    offsets = jnp.arange(N_WIDE, dtype=jnp.int32)[:, None] * TOK_DEV
    global_tokens = jnp.where(slot_tokens < TOK_DEV, slot_tokens + offsets, TOKENS).astype(jnp.int32)
    token_table = global_tokens.reshape(N_WIDE, EXPERTS, CAP).transpose(1, 0, 2).reshape(EXPERTS, N_WIDE * CAP)
    gate_table = slot_gates.reshape(N_WIDE, EXPERTS, CAP).transpose(1, 0, 2).reshape(EXPERTS, N_WIDE * CAP)
    return (token_table, gate_table)

def attention_forward_block(x_blk, seg_blk, attn_gain, w_query, w_latent, latent_gain, w_expand, w_output):
    x_float = x_blk.astype(jnp.float32)
    x_normed, inv_one = rms_forward(x_float, attn_gain)
    x_low = x_normed.astype(jnp.bfloat16)
    cos_tab, sin_tab = rotary_tables(positions(seg_blk))
    queries = jnp.dot(x_low, w_query, preferred_element_type=jnp.float32).reshape(TOK_DEV, H, DH + DR).transpose(1, 0, 2)
    q_heads = jnp.concatenate([queries[..., :DH], rotate(queries[..., DH:], cos_tab, sin_tab)], -1).astype(jnp.bfloat16)
    latent_all = jnp.dot(x_low, w_latent, preferred_element_type=jnp.float32)
    latent = latent_all[:, :KVR]
    latent_normed, inv_lat = rms_forward(latent, latent_gain)
    latent_low = latent_normed.astype(jnp.bfloat16)
    key_rope = rotate(latent_all[:, KVR:], cos_tab, sin_tab).astype(jnp.bfloat16)
    expanded = jnp.dot(latent_low, w_expand, preferred_element_type=jnp.float32).reshape(TOK_DEV, H, 2 * DH).transpose(1, 0, 2)
    key_nope = expanded[..., :DH].astype(jnp.bfloat16)
    v_heads = expanded[..., DH:].astype(jnp.bfloat16)
    k_heads = jnp.concatenate([key_nope, jnp.broadcast_to(key_rope[None], (H, TOK_DEV, DR))], -1)
    row_ids = jnp.arange(TOK_DEV, dtype=jnp.int32)
    attended, log_total = attend_forward(q_heads, k_heads, v_heads, seg_blk, seg_blk, row_ids, row_ids)
    merged = attended.transpose(1, 0, 2).reshape(TOK_DEV, H * DH)
    resid_sum = x_float + jnp.dot(merged, w_output, preferred_element_type=jnp.float32)
    return (resid_sum, (x_low, inv_one, q_heads, k_heads, v_heads, latent, inv_lat, latent_low, merged, log_total))

def attention_backward_block(grad_resid, x_blk, seg_blk, kept, attn_gain, w_query, w_latent, latent_gain, w_expand, w_output):
    x_low, inv_one, q_heads, k_heads, v_heads, latent, inv_lat, latent_low, merged, log_total = kept
    x_float = x_blk.astype(jnp.float32)
    cos_tab, sin_tab = rotary_tables(positions(seg_blk))
    row_ids = jnp.arange(TOK_DEV, dtype=jnp.int32)
    grad_low = grad_resid.astype(jnp.bfloat16)
    grad_merged = jnp.dot(grad_low, w_output.T, preferred_element_type=jnp.float32)
    grad_wo = jnp.dot(merged.T, grad_low, preferred_element_type=jnp.float32)
    grad_att = grad_merged.reshape(TOK_DEV, H, DH).transpose(1, 0, 2).astype(jnp.bfloat16)
    grad_q, grad_k, grad_v = attend_backward(q_heads, k_heads, v_heads, grad_att, log_total, seg_blk, seg_blk, row_ids, row_ids)
    grad_q_pre = jnp.concatenate([grad_q[..., :DH], unrotate(grad_q[..., DH:], cos_tab, sin_tab)], -1).astype(jnp.bfloat16)
    grad_q_pre = grad_q_pre.transpose(1, 0, 2).reshape(TOK_DEV, H * (DH + DR))
    grad_key_rope = lax.optimization_barrier(jnp.sum(grad_k[..., DH:], axis=0))
    grad_expanded = jnp.concatenate([grad_k[..., :DH], grad_v], -1).astype(jnp.bfloat16)
    grad_expanded = grad_expanded.transpose(1, 0, 2).reshape(TOK_DEV, H * 2 * DH)
    grad_wkvb = jnp.dot(latent_low.T, grad_expanded, preferred_element_type=jnp.float32)
    grad_latent_normed = jnp.dot(grad_expanded, w_expand.T, preferred_element_type=jnp.float32)
    grad_x_query = jnp.dot(grad_q_pre, w_query.T, preferred_element_type=jnp.float32)
    grad_wq = jnp.dot(x_low.T, grad_q_pre, preferred_element_type=jnp.float32)
    grad_latent, grad_lat_gain = rms_backward(latent, inv_lat, latent_gain, grad_latent_normed)
    grad_latent_all = jnp.concatenate([grad_latent, unrotate(grad_key_rope, cos_tab, sin_tab)], -1).astype(jnp.bfloat16)
    grad_wkva = jnp.dot(x_low.T, grad_latent_all, preferred_element_type=jnp.float32)
    grad_x_normed = grad_x_query + jnp.dot(grad_latent_all, w_latent.T, preferred_element_type=jnp.float32)
    grad_x, grad_att_gain = rms_backward(x_float, inv_one, attn_gain, grad_x_normed)
    return (grad_x + grad_resid, (grad_wq, grad_wkva, grad_wkvb, grad_wo, grad_att_gain, grad_lat_gain))

def reference(tokens_in, seg_ids, routes, gate_vals, attn_gain, w_query, w_latent, latent_gain, w_expand, w_output, ffn_gain, w_shared_in, w_shared_out, w_expert_in, w_expert_out, grad_output):
    x_blocks = tokens_in.reshape(N_WIDE, TOK_DEV, D)
    seg_blocks = seg_ids.reshape(N_WIDE, TOK_DEV)

    def forward_one(block_pair):
        return attention_forward_block(block_pair[0], block_pair[1], attn_gain, w_query, w_latent, latent_gain, w_expand, w_output)
    resid_blocks, kept = lax.map(forward_one, (x_blocks, seg_blocks))
    resid_sum = resid_blocks.reshape(TOKENS, D)
    resid_normed, inv_two = rms_forward(resid_sum, ffn_gain)
    hidden_low = resid_normed.astype(jnp.bfloat16)
    shin_flat = w_shared_in.reshape(D, 2 * SFF)
    shared_gu = jnp.dot(hidden_low, shin_flat, preferred_element_type=jnp.float32).reshape(TOKENS, 2, SFF)
    shared_act = swiglu(shared_gu).astype(jnp.bfloat16)
    shared_out = jnp.dot(shared_act, w_shared_out, preferred_element_type=jnp.float32)
    token_table, gate_table = expert_tables(routes, gate_vals)
    hidden_pad = jnp.concatenate([hidden_low, jnp.zeros((1, D), jnp.bfloat16)], 0)

    def expert_forward(total_rows, expert_item):
        w_in, w_out, idx_col, gate_col = expert_item
        rows_in = hidden_pad[idx_col]
        gate_up = jnp.dot(rows_in, w_in.reshape(D, 2 * FF), preferred_element_type=jnp.float32).reshape(-1, 2, FF)
        activated = swiglu(gate_up).astype(jnp.bfloat16)
        out_rows = jnp.dot(activated, w_out, preferred_element_type=jnp.float32)
        return (total_rows.at[idx_col].add(gate_col[:, None] * out_rows), None)
    routed_pad, unused = lax.scan(expert_forward, jnp.zeros((TOKENS + 1, D), jnp.float32), (w_expert_in, w_expert_out, token_table, gate_table))
    layer_out = (resid_sum + shared_out + routed_pad[:TOKENS]).astype(jnp.bfloat16)
    grad_out = grad_output.astype(jnp.float32)
    grad_shared_act = jnp.dot(grad_output, w_shared_out.T, preferred_element_type=jnp.float32)
    grad_shout = jnp.dot(shared_act.T, grad_output, preferred_element_type=jnp.float32)
    grad_shared_gu = swiglu_grad(shared_gu, grad_shared_act).astype(jnp.bfloat16).reshape(TOKENS, 2 * SFF)
    grad_shin = jnp.dot(hidden_low.T, grad_shared_gu, preferred_element_type=jnp.float32).reshape(D, 2, SFF)
    grad_hidden_shared = jnp.dot(grad_shared_gu, shin_flat.T, preferred_element_type=jnp.float32)
    grad_pad = jnp.concatenate([grad_out, jnp.zeros((1, D), jnp.float32)], 0)

    def expert_backward(total_rows, expert_item):
        w_in, w_out, idx_col, gate_col = expert_item
        rows_in = hidden_pad[idx_col]
        w_in_flat = w_in.reshape(D, 2 * FF)
        gate_up = jnp.dot(rows_in, w_in_flat, preferred_element_type=jnp.float32).reshape(-1, 2, FF)
        activated = swiglu(gate_up).astype(jnp.bfloat16)
        grad_rows_out = (gate_col[:, None] * grad_pad[idx_col]).astype(jnp.bfloat16)
        grad_act = jnp.dot(grad_rows_out, w_out.T, preferred_element_type=jnp.float32)
        grad_w_out = jnp.dot(activated.T, grad_rows_out, preferred_element_type=jnp.float32)
        grad_gu = swiglu_grad(gate_up, grad_act).astype(jnp.bfloat16).reshape(-1, 2 * FF)
        grad_w_in = jnp.dot(rows_in.T, grad_gu, preferred_element_type=jnp.float32).reshape(D, 2, FF)
        grad_in_rows = jnp.dot(grad_gu, w_in_flat.T, preferred_element_type=jnp.float32)
        return (total_rows.at[idx_col].add(grad_in_rows), (grad_w_in, grad_w_out))
    grad_routed_pad, expert_grads = lax.scan(expert_backward, jnp.zeros((TOKENS + 1, D), jnp.float32), (w_expert_in, w_expert_out, token_table, gate_table))
    grad_hidden = grad_hidden_shared + grad_routed_pad[:TOKENS]
    grad_resid, grad_ffn = rms_backward(resid_sum, inv_two, ffn_gain, grad_hidden)
    grad_resid = grad_resid + grad_out
    zero_grads = (jnp.zeros((D, H * (DH + DR)), jnp.float32), jnp.zeros((D, KVR + DR), jnp.float32), jnp.zeros((KVR, 2 * H * DH), jnp.float32), jnp.zeros((H * DH, D), jnp.float32), jnp.zeros((D,), jnp.float32), jnp.zeros((KVR,), jnp.float32))

    def backward_one(totals, block_item):
        grad_blk, x_blk, seg_blk, kept_blk = block_item
        grad_x, block_grads = attention_backward_block(grad_blk, x_blk, seg_blk, kept_blk, attn_gain, w_query, w_latent, latent_gain, w_expand, w_output)
        return (jax.tree.map(jnp.add, totals, block_grads), grad_x)
    totals, grad_x_blocks = lax.scan(backward_one, zero_grads, (grad_resid.reshape(N_WIDE, TOK_DEV, D), x_blocks, seg_blocks, kept))
    grad_wq, grad_wkva, grad_wkvb, grad_wo, grad_att_gain, grad_lat_gain = totals
    return (layer_out, grad_x_blocks.reshape(TOKENS, D), grad_att_gain, grad_wq, grad_wkva, grad_lat_gain, grad_wkvb, grad_wo, grad_ffn, grad_shin, grad_shout, expert_grads[0], expert_grads[1])
```

```python
import functools

import jax
import jax.numpy as jnp
from jax import lax
from jax.experimental import pallas as pl
from jax.experimental.pallas import tpu as pltpu
from jax.sharding import PartitionSpec as P

DH = 128
DR = 64
KVR = 512


EPS = 1e-06
THETA = 50000.0
NEG_BIG = -1e30
BLOCK_ROWS = 512


def positions(seg_ids):
    row_index = jnp.arange(seg_ids.shape[0], dtype=jnp.int32)
    starts = jnp.concatenate([jnp.ones((1,), dtype=bool), seg_ids[1:] != seg_ids[:-1]])
    begins = lax.cummax(jnp.where(starts, row_index, 0), axis=0)
    return (row_index - begins).astype(jnp.float32)


def rotary_tables(pos_float):
    half_dim = DR // 2
    inv_freq = THETA ** (-(jnp.arange(half_dim, dtype=jnp.float32) * 2.0 / DR))
    angles = pos_float[:, None] * inv_freq[None, :]
    return (jnp.cos(angles), jnp.sin(angles))


def rotate(values, cos_tab, sin_tab):
    half_dim = values.shape[-1] // 2
    lower_half = values[..., :half_dim]
    upper_half = values[..., half_dim:]
    return jnp.concatenate(
        [lower_half * cos_tab - upper_half * sin_tab, upper_half * cos_tab + lower_half * sin_tab],
        -1,
    )


def unrotate(values, cos_tab, sin_tab):
    half_dim = values.shape[-1] // 2
    lower_half = values[..., :half_dim]
    upper_half = values[..., half_dim:]
    return jnp.concatenate(
        [lower_half * cos_tab + upper_half * sin_tab, upper_half * cos_tab - lower_half * sin_tab],
        -1,
    )


def rms_forward(values, gain_vec):
    inv_rms = lax.rsqrt(jnp.mean(values * values, axis=-1, keepdims=True) + EPS)
    return (values * inv_rms * gain_vec, inv_rms)


def rms_backward(values, inv_rms, gain_vec, grad_out):
    scaled = grad_out * gain_vec
    grad_in = inv_rms * scaled - values * inv_rms**3 * jnp.mean(
        values * scaled, axis=-1, keepdims=True
    )
    grad_gain = jnp.sum(grad_out * values * inv_rms, axis=0)
    return (grad_in, grad_gain)


def masked_scores(q_blk, k_heads, seg_rows, seg_cols, row_pos, col_pos):
    scale = (DH + DR) ** (-0.5)
    scores = jnp.einsum("hqc,hkc->hqk", q_blk, k_heads, preferred_element_type=jnp.float32) * scale
    allowed = (seg_rows[:, None] == seg_cols[None, :]) & (col_pos[None, :] <= row_pos[:, None])
    return jnp.where(allowed[None], scores, NEG_BIG)


def attention_forward(q_heads, k_heads, v_heads, seg_ids):
    head_count = q_heads.shape[0]
    row_total = q_heads.shape[1]
    block_rows = min(row_total, BLOCK_ROWS)
    block_count = row_total // block_rows
    col_pos = jnp.arange(row_total, dtype=jnp.int32)

    def one_block(start):
        row_pos = start + jnp.arange(block_rows, dtype=jnp.int32)
        scores = masked_scores(q_heads, k_heads, seg_ids, seg_ids, row_pos, col_pos)
        top_score = jnp.max(scores, axis=-1, keepdims=True)
        log_total = top_score + jnp.log(
            jnp.sum(jnp.exp(scores - top_score), axis=-1, keepdims=True)
        )
        prob_low = jnp.exp(scores - log_total).astype(jnp.bfloat16)
        attended = jnp.einsum("hqk,hkd->hqd", prob_low, v_heads, preferred_element_type=jnp.float32)
        return (attended.astype(jnp.bfloat16), log_total)

    starts = jnp.arange(block_count, dtype=jnp.int32) * block_rows
    attended, log_total = lax.map(one_block, starts)
    attended = attended.transpose(1, 0, 2, 3).reshape(head_count, row_total, -1)
    log_total = log_total.transpose(1, 0, 2, 3).reshape(head_count, row_total, 1)
    return (attended, log_total)


def attention_backward(q_heads, k_heads, v_heads, grad_att, log_total, seg_ids):
    scale = (DH + DR) ** (-0.5)
    head_count = q_heads.shape[0]
    row_total = q_heads.shape[1]
    block_rows = min(row_total, BLOCK_ROWS)
    block_count = row_total // block_rows
    col_pos = jnp.arange(row_total, dtype=jnp.int32)

    def one_block(carry, start):
        grad_k_acc, grad_v_acc = carry
        row_pos = start + jnp.arange(block_rows, dtype=jnp.int32)
        scores = masked_scores(q_heads, k_heads, seg_ids, seg_ids, row_pos, col_pos)
        prob_full = jnp.exp(scores - log_total)
        prob_low = prob_full.astype(jnp.bfloat16)
        grad_v_blk = jnp.einsum(
            "hqk,hqd->hkd", prob_low, grad_att, preferred_element_type=jnp.float32
        )
        grad_prob = jnp.einsum(
            "hqd,hkd->hqk", grad_att, v_heads, preferred_element_type=jnp.float32
        )
        row_dot = jnp.sum(prob_full * grad_prob, axis=-1, keepdims=True)
        grad_scores = (prob_full * (grad_prob - row_dot) * scale).astype(jnp.bfloat16)
        grad_q_blk = jnp.einsum(
            "hqk,hkc->hqc", grad_scores, k_heads, preferred_element_type=jnp.float32
        )
        grad_k_blk = jnp.einsum(
            "hqk,hqc->hkc", grad_scores, q_heads, preferred_element_type=jnp.float32
        )
        return ((grad_k_acc + grad_k_blk, grad_v_acc + grad_v_blk), grad_q_blk)

    starts = jnp.arange(block_count, dtype=jnp.int32) * block_rows
    init_acc = (jnp.zeros(k_heads.shape, jnp.float32), jnp.zeros(v_heads.shape, jnp.float32))
    (grad_k, grad_v), grad_q_blocks = lax.scan(one_block, init_acc, starts)
    grad_q = grad_q_blocks.transpose(1, 0, 2, 3).reshape(head_count, row_total, -1)
    return (grad_q, grad_k, grad_v)


MESH_IDS = pl.DeviceIdType.MESH


def axis_parts(mesh):
    devices = mesh.devices
    found = []
    for axis in range(devices.ndim):
        line = [devices[tuple(i if k == axis else 0 for k in range(devices.ndim))] for i in range(devices.shape[axis])]
        places = [(*dev.coords, dev.core_on_chip) for dev in line]
        parts = []
        for k, name in enumerate(("x", "y", "z", "core")):
            values = [p[k] for p in places]
            size = len(set(values))
            if size > 1:
                stride = next(i for i, v in enumerate(values) if v != values[0])
                parts.append((stride, name, size))
        found.append(tuple((name, size) for stride, name, size in sorted(parts, reverse=True)))
    return tuple(found)


def fits_kernels(mesh):
    (wide, narrow) = axis_parts(mesh)
    return (
        len(wide) == 2
        and wide[1][1] == 2
        and len(narrow) == 2
        and narrow[0][1] == 2
        and narrow[1] == ("core", 2)
    )


class Spot:
    def __init__(self, line):
        wide, narrow = lax.axis_index("wide"), lax.axis_index("narrow")
        self.line = line
        self.z, self.x = wide // 2, wide % 2
        self.y, self.c = narrow // 2, narrow % 2

    def flips(self, a, b, c):
        return a * (1 - c) + b * c, b * (1 - c) + a * c

    def at(self, z, a, b, c):
        fx, fy = self.flips(a, b, c)
        x = self.x + fx * (1 - 2 * self.x)
        y = self.y + fy * (1 - 2 * self.y)
        return z * 2 + x, y * 2 + c

    def device(self, z, a, b, c):
        wide, narrow = self.at(z, a, b, c)
        return {"wide": wide, "narrow": narrow}

    def inside(self, z):
        return (z >= 0) & (z < self.line)


def gather_offsets(kind, line):
    ks = [(0, 0)] if kind == "narrow" else [(0, 0)] + [(d, k) for k in range(1, line) for d in (1, -1)]
    out = []
    for d, k in ks:
        for a in (0, 1):
            if kind == "narrow" and a:
                continue
            for b in (0, 1):
                if kind == "wide" and b:
                    continue
                level = k + a + (2 if b else 0) + (a if b else 0)
                out.append((level, d, k, a, b))
    return sorted(out, key=lambda o: (o[0], o[3], o[4], o[2]))


def sends_of(kind, d, k, a, b):
    to = []
    if not a and not b and kind != "narrow":
        to += [("z", 1), ("z", -1)] if k == 0 else [("z", d)]
    if kind in ("all", "wide") and not a and not b:
        to.append(("a", 0))
    if kind in ("all", "narrow") and not b:
        to.append(("b", 0))
    if kind in ("all", "narrow"):
        to.append(("core", 0))
    return to


def count_sends(kind, line):
    return sum(len(sends_of(kind, *o[1:])) for o in gather_offsets(kind, line))


def gather_kernel(line, kinds, views, *refs):
    count = len(kinds)
    srcs, dsts = refs[:count], refs[count : 2 * count]
    sends, recvs, local = refs[2 * count : 3 * count], refs[3 * count : 4 * count], refs[4 * count]
    spot = Spot(line)
    z, c = spot.z, spot.c
    use_line = any(kind != "narrow" for kind in kinds)
    pairs = set()
    for kind in kinds:
        pairs |= {"all": {(1, 0, 0), (0, 1, 0), (0, 0, 1)}, "wide": {(1, 0, 0)}, "narrow": {(0, 1, 0), (0, 0, 1)}}[kind]
    greet_pairs = sorted(pairs)

    def color(kind):
        return c if kind == "all" else 0

    def target(kind, move, step):
        if kind == "all":
            where = {"z": (z + step, 0, 0, c), "a": (z, 1, 0, c), "b": (z, 0, 1, c), "core": (z, 0, 0, 1 - c)}[move]
            return spot.device(*where)
        wide, narrow = z * 2 + spot.x, spot.y * 2 + c
        if move == "z":
            return {"wide": wide + 2 * step, "narrow": narrow}
        if move == "a":
            return {"wide": z * 2 + 1 - spot.x, "narrow": narrow}
        if move == "b":
            return {"wide": wide, "narrow": (1 - spot.y) * 2 + c}
        return {"wide": wide, "narrow": spot.y * 2 + 1 - c}

    def origin(kind, zz, a, b, flip):
        if kind == "all":
            wide, narrow = spot.at(zz, a, b, c) if not flip else spot.at(zz, a, b, 1 - c)
            return wide * 4 + narrow
        if kind == "wide":
            return zz * 2 + spot.x + a * (1 - 2 * spot.x)
        return (spot.y + b * (1 - 2 * spot.y)) * 2 + c + flip * (1 - 2 * c)

    def move_of(i, block, first, move, step, number):
        view = views[i](dsts[i], block)
        return pltpu.make_async_remote_copy(
            src_ref=srcs[i] if first else view,
            dst_ref=view,
            send_sem=sends[i].at[number],
            recv_sem=recvs[i].at[block],
            device_id=target(kinds[i], move, step),
            device_id_type=MESH_IDS,
        )

    barrier = pltpu.get_barrier_semaphore()
    total = 0
    for a, b, flip in greet_pairs:
        dev = {"wide": z * 2 + spot.x + a * (1 - 2 * spot.x), "narrow": (spot.y + b * (1 - 2 * spot.y)) * 2 + c + flip * (1 - 2 * c)}
        pl.semaphore_signal(barrier, inc=1, device_id=dev, device_id_type=MESH_IDS)
        total += 1
    if use_line:
        for step in (-1, 1):
            @pl.when(spot.inside(z + step))
            def _():
                dev = {"wide": (z + step) * 2 + spot.x, "narrow": spot.y * 2 + c}
                pl.semaphore_signal(barrier, inc=1, device_id=dev, device_id_type=MESH_IDS)
        inner = spot.inside(z - 1) & spot.inside(z + 1)
        @pl.when(inner)
        def _():
            pl.semaphore_wait(barrier, total + 2)
        @pl.when(jnp.logical_not(inner))
        def _():
            pl.semaphore_wait(barrier, total + 1)
    else:
        pl.semaphore_wait(barrier, total)

    own_copies = []
    for i, kind in enumerate(kinds):
        own_copies.append(pltpu.make_async_copy(srcs[i], views[i](dsts[i], origin(kind, z, 0, 0, 0)), local.at[i]))
        own_copies[-1].start()

    pending = []
    plans = [(level, i, (d, k, a, b)) for i, kind in enumerate(kinds) for level, d, k, a, b in gather_offsets(kind, line)]
    numbers = [0] * count
    plans.sort(key=lambda p: p[0])
    for level, i, (d, k, a, b) in plans:
        kind = kinds[i]
        zz = z - d * k
        block = origin(kind, zz, a, b, 0)
        first = k == 0 and not a and not b
        outs = []
        for move, step in sends_of(kind, d, k, a, b):
            outs.append((move, step, numbers[i]))
            numbers[i] += 1

        def act(i=i, block=block, first=first, outs=outs, zz=zz):
            if not first:
                view = views[i](dsts[i], block)
                pltpu.make_async_remote_copy(
                    src_ref=view, dst_ref=view, send_sem=sends[i].at[0], recv_sem=recvs[i].at[block],
                    device_id=target(kinds[i], "core" if kinds[i] != "wide" else "a", 0), device_id_type=MESH_IDS,
                ).wait_recv()
            for move, step, number in outs:
                if move == "z":
                    @pl.when(spot.inside(z + step))
                    def _():
                        move_of(i, block, first, move, step, number).start()
                else:
                    move_of(i, block, first, move, step, number).start()

        def finish(i=i, block=block, first=first, outs=outs):
            for move, step, number in outs:
                if move == "z":
                    @pl.when(spot.inside(z + step))
                    def _():
                        move_of(i, block, first, move, step, number).wait_send()
                else:
                    move_of(i, block, first, move, step, number).wait_send()

        if k == 0:
            act()
        else:
            pl.when(spot.inside(zz))(act)
        pending.append((k, zz, finish))

    for i, kind in enumerate(kinds):
        if kind == "wide":
            continue
        for zz in range(line) if kind == "all" else (0,):
            for a in (0, 1) if kind == "all" else (0,):
                for b in (0, 1):
                    block = origin(kind, zz, a, b, 1)
                    view = views[i](dsts[i], block)
                    pltpu.make_async_remote_copy(
                        src_ref=view, dst_ref=view, send_sem=sends[i].at[0], recv_sem=recvs[i].at[block],
                        device_id=target(kind, "core", 0), device_id_type=MESH_IDS,
                    ).wait_recv()
    for k, zz, finish in pending:
        if k == 0:
            finish()
        else:
            pl.when(spot.inside(zz))(finish)
    for copy in own_copies:
        copy.wait()


def gather(line, items, collective_id):
    kinds = [kind for _, kind, _ in items]
    counts = {"all": line * 8, "wide": line * 2, "narrow": 4}

    def view_of(shape, axis):
        if axis == "grid":
            rows, cols = shape

            def tile(ref, block):
                at_row = pl.multiple_of((block % 4) * rows, rows)
                at_col = pl.multiple_of((block // 4) * cols, cols)
                return ref.at[pl.ds(at_row, rows), pl.ds(at_col, cols)]

            return tile
        size = shape[axis]

        def view(ref, block):
            at = pl.ds(pl.multiple_of(block * size, size), size)
            return ref.at[tuple(at if k == axis else slice(None) for k in range(len(shape)))]

        return view

    views = [view_of(arr.shape, axis) for arr, _, axis in items]
    def whole(arr, kind, axis):
        if axis == "grid":
            return (arr.shape[0] * 4, arr.shape[1] * line * 2)
        return tuple(s * counts[kind] if k == axis else s for k, s in enumerate(arr.shape))

    shapes = [jax.ShapeDtypeStruct(whole(*item), item[0].dtype) for item in items]
    moved = sum((counts[kind] - 1) * arr.size * arr.dtype.itemsize for arr, kind, _ in items)
    return pl.pallas_call(
        functools.partial(gather_kernel, line, kinds, views),
        out_shape=shapes,
        in_specs=[pl.BlockSpec(memory_space=pltpu.VMEM)] * len(items),
        out_specs=[pl.BlockSpec(memory_space=pl.ANY)] * len(items),
        scratch_shapes=[pltpu.SemaphoreType.DMA((count_sends(kind, line),)) for kind in kinds]
        + [pltpu.SemaphoreType.DMA((counts[kind],)) for kind in kinds]
        + [pltpu.SemaphoreType.DMA((len(items),))],
        compiler_params=pltpu.CompilerParams(collective_id=collective_id, has_side_effects=True),
        cost_estimate=pl.CostEstimate(flops=0, bytes_accessed=moved, transcendentals=0),
        name="gather_blocks",
    )(*[arr for arr, _, _ in items])


def reduce_kernel(line, kind, rows, part, out, held, summed, from_core, from_b, from_a, from_z,
                  load_sem, core_send, core_recv, b_send, b_recv, a_send, a_recv, z_send, z_recv):
    spot = Spot(line)
    z, c = spot.z, spot.c
    full = kind == "all"
    zs = range(line) if full else (0,)
    flags = (0, 1) if full else (0,)

    def where(zz, a, b, cc):
        if full:
            wide, narrow = spot.at(zz, a, b, cc)
            return wide * 4 + narrow
        return (spot.y + b * (1 - 2 * spot.y)) * 2 + cc

    def device(zz, a, b, cc):
        if full:
            return spot.device(zz, a, b, cc)
        return {"wide": lax.axis_index("wide"), "narrow": (spot.y + b * (1 - 2 * spot.y)) * 2 + cc}

    def block(ref, index):
        return ref.at[pl.ds(pl.multiple_of(index * rows, rows), rows), :]

    def slot(zz, a, b):
        return (zz * 2 + a) * 2 + b if full else b

    barrier = pltpu.get_barrier_semaphore()
    total = 0
    if full:
        pl.semaphore_signal(barrier, inc=1, device_id=device(z, 1, 0, c), device_id_type=MESH_IDS)
        total += 1
    pl.semaphore_signal(barrier, inc=1, device_id=device(z, 0, 1, c), device_id_type=MESH_IDS)
    pl.semaphore_signal(barrier, inc=1, device_id=device(z, 0, 0, 1 - c), device_id_type=MESH_IDS)
    total += 2
    if full:
        for step in (-1, 1):
            @pl.when(spot.inside(z + step))
            def _():
                pl.semaphore_signal(barrier, inc=1, device_id=device(z + step, 0, 0, c), device_id_type=MESH_IDS)
        inner = spot.inside(z - 1) & spot.inside(z + 1)
        @pl.when(inner)
        def _():
            pl.semaphore_wait(barrier, total + 2)
        @pl.when(jnp.logical_not(inner))
        def _():
            pl.semaphore_wait(barrier, total + 1)
    else:
        pl.semaphore_wait(barrier, total)

    if full:
        steps = [(d, k) for k in range(line - 1, 0, -1) for d in (1, -1)] + [(0, 0)]
    else:
        steps = [(0, 0)]
    order = [(b, a, d, k) for b in (1, 0) for a in reversed(flags) for d, k in steps]

    def to_core(zz, a, b):
        return pltpu.make_async_remote_copy(
            src_ref=block(part, where(zz, a, b, 1 - c)), dst_ref=from_core.at[slot(zz, a, b)],
            send_sem=core_send.at[slot(zz, a, b)], recv_sem=core_recv.at[slot(zz, a, b)],
            device_id=device(z, 0, 0, 1 - c), device_id_type=MESH_IDS,
        )

    def load(zz, a, b):
        return pltpu.make_async_copy(
            block(part, where(zz, a, b, c)), held.at[slot(zz, a, b)], load_sem.at[slot(zz, a, b)]
        )

    def to_b(zz, a):
        return pltpu.make_async_remote_copy(
            src_ref=summed.at[slot(zz, a, 1)], dst_ref=from_b.at[zz * 2 + a],
            send_sem=b_send.at[zz * 2 + a], recv_sem=b_recv.at[zz * 2 + a],
            device_id=device(z, 0, 1, c), device_id_type=MESH_IDS,
        )

    def to_a(zz):
        return pltpu.make_async_remote_copy(
            src_ref=summed.at[slot(zz, 1, 0)], dst_ref=from_a.at[zz],
            send_sem=a_send.at[zz], recv_sem=a_recv.at[zz],
            device_id=device(z, 1, 0, c), device_id_type=MESH_IDS,
        )

    def to_z(zz, d):
        way = (1 - d) // 2
        return pltpu.make_async_remote_copy(
            src_ref=summed.at[slot(zz, 0, 0)], dst_ref=from_z.at[way * line + zz],
            send_sem=z_send.at[zz], recv_sem=z_recv.at[way * line + zz],
            device_id=device(z + d, 0, 0, c), device_id_type=MESH_IDS,
        )

    def guarded(k, zz, act):
        if k == 0:
            act()
        else:
            pl.when(spot.inside(zz))(act)

    for b, a, d, k in order:
        zz = z + d * k if full else 0
        guarded(k, zz, lambda: (to_core(zz, a, b).start(), load(zz, a, b).start()) and None)

    for b, a, d, k in order:
        zz = z + d * k if full else 0

        def act():
            at = slot(zz, a, b)
            load(zz, a, b).wait()
            to_core(zz, a, b).wait_recv()
            value = held[at].astype(jnp.float32) + from_core[at].astype(jnp.float32)
            if b == 1:
                summed[at] = value.astype(summed.dtype)
                to_b(zz, a).start()
                return
            to_b(zz, a).wait_recv()
            value = value + from_b[zz * 2 + a].astype(jnp.float32)
            if a == 1:
                summed[at] = value.astype(summed.dtype)
                to_a(zz).start()
                return
            if full:
                to_a(zz).wait_recv()
                value = value + from_a[zz].astype(jnp.float32)
            if k:
                way = (1 - d) // 2
                summed[at] = value.astype(summed.dtype)
                @pl.when(spot.inside(z - d))
                def _():
                    to_z(zz, d).wait_recv()
                    summed[at] = (value + from_z[way * line + zz].astype(jnp.float32)).astype(summed.dtype)
                to_z(zz, d).start()
                return
            out[...] = value
            if full:
                for way_d in (1, -1):
                    @pl.when(spot.inside(z - way_d))
                    def _():
                        way = (1 - way_d) // 2
                        to_z(z, way_d).wait_recv()
                        out[...] += from_z[way * line + z].astype(jnp.float32)

        guarded(k, zz, act)

    for b, a, d, k in order:
        zz = z + d * k if full else 0

        def act():
            to_core(zz, a, b).wait_send()
            if b == 1:
                to_b(zz, a).wait_send()
            elif a == 1:
                to_a(zz).wait_send()
            elif k:
                to_z(zz, d).wait_send()

        guarded(k, zz, act)


def reduce_blocks(line, kind, part, collective_id):
    full = kind == "all"
    blocks = line * 8 if full else 4
    rows, width = part.shape[0] // blocks, part.shape[1]
    zs = line if full else 1
    slots = zs * 4 if full else 2
    dma = pltpu.SemaphoreType.DMA
    low = part.dtype
    return pl.pallas_call(
        functools.partial(reduce_kernel, line, kind, rows),
        out_shape=jax.ShapeDtypeStruct((rows, width), jnp.float32),
        in_specs=[pl.BlockSpec(memory_space=pl.ANY)],
        out_specs=pl.BlockSpec(memory_space=pltpu.VMEM),
        scratch_shapes=[
            pltpu.VMEM((slots, rows, width), low),
            pltpu.VMEM((slots, rows, width), low),
            pltpu.VMEM((slots, rows, width), low),
            pltpu.VMEM((zs * 2, rows, width), low),
            pltpu.VMEM((zs, rows, width), low),
            pltpu.VMEM((2 * zs, rows, width), low),
            dma((slots,)),
            dma((slots,)),
            dma((slots,)),
            dma((zs * 2,)),
            dma((zs * 2,)),
            dma((zs,)),
            dma((zs,)),
            dma((zs,)),
            dma((2 * zs,)),
        ],
        compiler_params=pltpu.CompilerParams(collective_id=collective_id, has_side_effects=True),
        cost_estimate=pl.CostEstimate(
            flops=part.size, bytes_accessed=2 * part.size * part.dtype.itemsize, transcendentals=0
        ),
        name="sum_blocks",
    )(part)

class Links:
    AXES = {"all": ("wide", "narrow"), "wide": "wide", "narrow": "narrow"}

    def __init__(self, mesh):
        self.line = axis_parts(mesh)[0][0][1] if fits_kernels(mesh) else None
        self.calls = 0

    def gather(self, *items):
        if self.line:
            self.calls += 1
            return gather(self.line, items, self.calls)
        return [self.plain(*item) for item in items]

    def plain(self, arr, kind, axis):
        if axis == "grid":
            return lax.all_gather(self.plain(arr, "narrow", 0), "wide", axis=1, tiled=True)
        return lax.all_gather(arr, self.AXES[kind], axis=axis, tiled=True)

    def reduce(self, kind, part):
        if self.line:
            self.calls += 1
            return reduce_blocks(self.line, kind, part, self.calls)
        summed = lax.psum_scatter(part, self.AXES[kind], scatter_dimension=0, tiled=True)
        return summed.astype(jnp.float32)


def rows_of(array, index, count):
    return lax.dynamic_slice_in_dim(array, index * count, count, 0)


def dot_nt(lhs, rhs):
    return lax.dot_general(lhs, rhs, (((1,), (1,)), ((), ())), preferred_element_type=jnp.float32)


def dot_tn(lhs, rhs):
    return lax.dot_general(lhs, rhs, (((0,), (0,)), ((), ())), preferred_element_type=jnp.float32)


def dot_nn(lhs, rhs):
    return jnp.dot(lhs, rhs, preferred_element_type=jnp.float32)


def per_device(
    links,
    tokens_in,
    seg_ids,
    routes,
    gate_vals,
    attn_gain,
    w_query,
    w_latent,
    latent_gain,
    w_expand,
    w_output,
    ffn_gain,
    w_shared_in,
    w_shared_out,
    w_expert_in,
    w_expert_out,
    grad_output,
):
    links.calls = 0
    both = ("wide", "narrow")
    low = jnp.bfloat16
    wide_count = lax.axis_size("wide")
    narrow_count = lax.axis_size("narrow")
    wide_at = lax.axis_index("wide")
    narrow_at = lax.axis_index("narrow")
    tok_rows, width = tokens_in.shape
    own_rows = tok_rows // narrow_count
    local_experts = w_expert_in.shape[0]
    hidden_local = w_expert_in.shape[3]
    num_experts = local_experts * wide_count
    head_local = w_query.shape[1] // (DH + DR)
    shared_local = w_shared_out.shape[0] // wide_count

    def mine(array):
        return rows_of(array, narrow_at, own_rows)

    latent_part = rows_of(w_latent.T, narrow_at, w_latent.shape[1] // narrow_count)
    wq_all, wkva_all, wkvb_all, wo_all = links.gather(
        (w_query, "wide", 0), (latent_part, "all", "grid"), (w_expand, "wide", 0), (w_output, "wide", 1)
    )
    grad_all = lax.all_gather(mine(grad_output), both, axis=0, tiled=True)
    shared_in = lax.all_to_all(
        w_shared_in.transpose(1, 2, 0), "wide", split_axis=1, concat_axis=2, tiled=True
    )
    shared_out = lax.all_to_all(w_shared_out, "wide", split_axis=0, concat_axis=1, tiled=True)
    chosen = routes[:, :, None] == jnp.arange(num_experts, dtype=jnp.int32)
    gate_table = jnp.sum(jnp.where(chosen, gate_vals[:, :, None], 0.0), axis=1)
    gates = lax.all_to_all(gate_table, "wide", split_axis=1, concat_axis=0, tiled=True).T

    x_float = tokens_in.astype(jnp.float32)
    x_normed, inv_one = rms_forward(x_float, attn_gain)
    x_low = x_normed.astype(low)
    x_cols = lax.all_to_all(x_low, "wide", split_axis=1, concat_axis=0, tiled=True)
    cos_tab, sin_tab = rotary_tables(positions(seg_ids))
    queries = dot_nn(x_low, wq_all).reshape(tok_rows, head_local, DH + DR).transpose(1, 0, 2)
    q_heads = jnp.concatenate(
        [queries[..., :DH], rotate(queries[..., DH:], cos_tab, sin_tab)], -1
    ).astype(low)
    latent_all = dot_nt(x_low, wkva_all)
    latent = latent_all[:, :KVR]
    latent_normed, inv_lat = rms_forward(latent, latent_gain)
    latent_low = latent_normed.astype(low)
    key_rope = rotate(latent_all[:, KVR:], cos_tab, sin_tab).astype(low)
    expanded = dot_nn(latent_low, wkvb_all).reshape(tok_rows, head_local, 2 * DH).transpose(1, 0, 2)
    key_nope = expanded[..., :DH].astype(low)
    v_heads = expanded[..., DH:].astype(low)
    k_heads = jnp.concatenate(
        [key_nope, jnp.broadcast_to(key_rope[None], (head_local, tok_rows, DR))], -1
    )
    attended, log_total = attention_forward(q_heads, k_heads, v_heads, seg_ids)
    merged = attended.transpose(1, 0, 2).reshape(tok_rows, head_local * DH)
    mixed_part = dot_nn(merged, wo_all).astype(low)
    mixed = links.reduce("narrow", mixed_part)

    x_rows = mine(x_float)
    inv_one_rows = mine(inv_one)
    resid = x_rows + mixed
    resid_normed, inv_two = rms_forward(resid, ffn_gain)
    (hidden,) = links.gather((resid_normed.astype(low), "all", 0))

    expert_rows = local_experts * hidden_local
    w_gate_up = w_expert_in.transpose(0, 2, 3, 1)
    expert_gu = dot_nt(w_gate_up.reshape(2 * expert_rows, width), hidden)
    expert_gu = expert_gu.reshape(local_experts, 2, hidden_local, -1)
    shared_gu = dot_nt(shared_in.reshape(2 * shared_local, width), hidden)
    shared_gu = shared_gu.reshape(2, shared_local, -1)
    down = jnp.concatenate([w_expert_out.reshape(expert_rows, width), shared_out], 0)
    grad_act = dot_nt(down, grad_all)
    grad_act_exp = grad_act[:expert_rows].reshape(local_experts, hidden_local, -1)
    grad_act_exp = grad_act_exp * gates[:, None, :]
    grad_act_sh = grad_act[expert_rows:]

    def both_ways(gate_part, up_part, grad_part):
        sig = jax.nn.sigmoid(gate_part)
        act = gate_part * sig * up_part
        grad_gate = grad_part * up_part * sig * (1.0 + gate_part * (1.0 - sig))
        grad_up = grad_part * gate_part * sig
        return act, grad_gate.astype(low), grad_up.astype(low)

    act_exp, dgate_exp, dup_exp = both_ways(expert_gu[:, 0], expert_gu[:, 1], grad_act_exp)
    act_sh, dgate_sh, dup_sh = both_ways(shared_gu[0], shared_gu[1], grad_act_sh)
    act_exp = (act_exp * gates[:, None, :]).astype(low).reshape(expert_rows, -1)
    act_all = jnp.concatenate([act_exp, act_sh.astype(low)], 0)
    grad_gu_exp = jnp.stack([dgate_exp, dup_exp], 1).reshape(2 * expert_rows, -1)
    grad_gu_sh = jnp.stack([dgate_sh, dup_sh], 0).reshape(2 * shared_local, -1)

    grad_hidden = dot_tn(grad_gu_exp, w_gate_up.reshape(2 * expert_rows, width)) + dot_tn(
        grad_gu_sh, shared_in.reshape(2 * shared_local, width)
    )
    grad_hidden = links.reduce("all", grad_hidden.astype(low))
    out_part = dot_tn(act_all, down)
    out_rows = lax.psum_scatter(out_part.astype(low), both, scatter_dimension=0, tiled=True)
    grad_down = dot_nn(act_all, grad_all)
    grad_exp_out = grad_down[:expert_rows].reshape(local_experts, hidden_local, width)
    red_shout = lax.all_to_all(
        grad_down[expert_rows:].astype(low), "wide", split_axis=1, concat_axis=0, tiled=True
    ).astype(jnp.float32)
    grad_exp_in = dot_nn(grad_gu_exp, hidden).reshape(local_experts, 2, hidden_local, width)
    grad_exp_in = grad_exp_in.transpose(0, 3, 1, 2)
    grad_shin = dot_nn(grad_gu_sh, hidden).reshape(2, shared_local, width).astype(low)
    red_shin = lax.all_to_all(grad_shin, "wide", split_axis=2, concat_axis=1, tiled=True)
    red_shin = red_shin.astype(jnp.float32).transpose(2, 0, 1)

    out_rows = (resid + out_rows.astype(jnp.float32)).astype(low)
    layer_out = lax.all_to_all(out_rows, "narrow", split_axis=1, concat_axis=0, tiled=True)

    grad_resid, grad_ffn = rms_backward(resid, inv_two, ffn_gain, grad_hidden)
    grad_resid = grad_resid + mine(grad_output).astype(jnp.float32)
    (grad_low,) = links.gather((grad_resid.astype(low), "narrow", 0))
    grad_merged = dot_nt(grad_low, wo_all)
    grad_wo = dot_tn(merged, grad_low).astype(low)
    red_wo = lax.psum_scatter(grad_wo, "wide", scatter_dimension=1, tiled=True)
    grad_att = grad_merged.reshape(tok_rows, head_local, DH).transpose(1, 0, 2).astype(low)
    grad_q, grad_k, grad_v = attention_backward(
        q_heads, k_heads, v_heads, grad_att, log_total, seg_ids
    )
    grad_q_pre = jnp.concatenate(
        [grad_q[..., :DH], unrotate(grad_q[..., DH:], cos_tab, sin_tab)], -1
    ).astype(low)
    grad_q_pre = grad_q_pre.transpose(1, 0, 2).reshape(tok_rows, head_local * (DH + DR))
    grad_rope_part = jnp.sum(grad_k[..., DH:], axis=0)
    grad_expanded = jnp.concatenate([grad_k[..., :DH], grad_v], -1).astype(low)
    grad_expanded = grad_expanded.transpose(1, 0, 2).reshape(tok_rows, head_local * 2 * DH)
    grad_latent_part = dot_nt(grad_expanded, wkvb_all)
    grad_x_part = dot_nt(grad_q_pre, wq_all)
    terms = jnp.concatenate([grad_x_part, grad_latent_part, grad_rope_part], 1)
    terms = links.reduce("narrow", terms.astype(low))
    grad_x_query, latent_terms = terms[:, :width], terms[:, width:]
    grad_wkvb = dot_tn(latent_low, grad_expanded).astype(low)
    red_wkvb = lax.psum_scatter(grad_wkvb, "wide", scatter_dimension=0, tiled=True)
    grad_latent, grad_lat_gain = rms_backward(
        mine(latent), mine(inv_lat), latent_gain, latent_terms[:, :KVR]
    )
    grad_rope = unrotate(latent_terms[:, KVR:], mine(cos_tab), mine(sin_tab))
    grad_latent_all = jnp.concatenate([grad_latent, grad_rope], -1).astype(low)
    grad_x_normed = grad_x_query + dot_nn(grad_latent_all, wkva_all)
    grad_x, grad_att_gain = rms_backward(x_rows, inv_one_rows, attn_gain, grad_x_normed)
    grad_tokens = (grad_x + grad_resid).astype(low)
    q_pre_all, latent_rows, grad_tokens = links.gather(
        (grad_q_pre, "wide", 0), (grad_latent_all, "all", 0), (grad_tokens, "narrow", 0)
    )
    grad_tokens = grad_tokens.astype(jnp.float32)
    red_wkva = dot_tn(x_cols, latent_rows)
    red_wq = dot_tn(x_cols, q_pre_all)
    gains = jnp.concatenate(
        [part.reshape(wide_count, -1) for part in (grad_att_gain, grad_ffn, grad_lat_gain)], 1
    )
    gains = lax.dynamic_index_in_dim(lax.psum(gains, both), wide_at, 0, keepdims=False)
    part = width // wide_count
    red_att_gain, red_ffn, red_lat_gain = gains[:part], gains[part : 2 * part], gains[2 * part :]
    return (
        layer_out,
        grad_tokens,
        red_att_gain,
        red_wq,
        red_wkva,
        red_lat_gain,
        red_wkvb.astype(jnp.float32),
        red_wo.astype(jnp.float32),
        red_ffn,
        red_shin,
        red_shout,
        grad_exp_in,
        grad_exp_out,
    )


def solution(mesh):
    placed = (
        P("wide", None),
        P("wide"),
        P("wide", None),
        P("wide", None),
        P(),
        P("wide", "narrow"),
        P("wide", None),
        P(),
        P("wide", "narrow"),
        P("narrow", "wide"),
        P(),
        P("wide", None, "narrow"),
        P("narrow", "wide"),
        P("wide", None, None, "narrow"),
        P("wide", "narrow", None),
        P("wide", None),
    )
    return jax.shard_map(
        functools.partial(per_device, Links(mesh)),
        mesh=mesh,
        in_specs=placed,
        out_specs=(
            P("wide", "narrow"),
            P("wide", None),
            P("wide"),
            P("wide", "narrow"),
            P("wide", None),
            P("wide"),
            P("wide", "narrow"),
            P("narrow", "wide"),
            P("wide"),
            P("wide", None, "narrow"),
            P("narrow", "wide"),
            P("wide", None, None, "narrow"),
            P("wide", "narrow", None),
        ),
        check_vma=False,
    )
```

```python
import functools

import jax
import jax.numpy as jnp
from jax import lax
from jax.experimental import pallas as pl
from jax.experimental.pallas import tpu as pltpu
from jax.sharding import PartitionSpec as P

DH = 128
DR = 64
KVR = 512


EPS = 1e-06
THETA = 50000.0
NEG_BIG = -1e30
BLOCK_ROWS = 512


def positions(seg_ids):
    row_index = jnp.arange(seg_ids.shape[0], dtype=jnp.int32)
    starts = jnp.concatenate([jnp.ones((1,), dtype=bool), seg_ids[1:] != seg_ids[:-1]])
    begins = lax.cummax(jnp.where(starts, row_index, 0), axis=0)
    return (row_index - begins).astype(jnp.float32)


def rotary_tables(pos_float):
    half_dim = DR // 2
    inv_freq = THETA ** (-(jnp.arange(half_dim, dtype=jnp.float32) * 2.0 / DR))
    angles = pos_float[:, None] * inv_freq[None, :]
    return (jnp.cos(angles), jnp.sin(angles))


def rotate(values, cos_tab, sin_tab):
    half_dim = values.shape[-1] // 2
    lower_half = values[..., :half_dim]
    upper_half = values[..., half_dim:]
    return jnp.concatenate(
        [lower_half * cos_tab - upper_half * sin_tab, upper_half * cos_tab + lower_half * sin_tab],
        -1,
    )


def unrotate(values, cos_tab, sin_tab):
    half_dim = values.shape[-1] // 2
    lower_half = values[..., :half_dim]
    upper_half = values[..., half_dim:]
    return jnp.concatenate(
        [lower_half * cos_tab + upper_half * sin_tab, upper_half * cos_tab - lower_half * sin_tab],
        -1,
    )


def rms_forward(values, gain_vec):
    inv_rms = lax.rsqrt(jnp.mean(values * values, axis=-1, keepdims=True) + EPS)
    return (values * inv_rms * gain_vec, inv_rms)


def rms_backward(values, inv_rms, gain_vec, grad_out):
    scaled = grad_out * gain_vec
    grad_in = inv_rms * scaled - values * inv_rms**3 * jnp.mean(
        values * scaled, axis=-1, keepdims=True
    )
    grad_gain = jnp.sum(grad_out * values * inv_rms, axis=0)
    return (grad_in, grad_gain)


def masked_scores(q_blk, k_heads, seg_rows, seg_cols, row_pos, col_pos):
    scale = (DH + DR) ** (-0.5)
    scores = jnp.einsum("hqc,hkc->hqk", q_blk, k_heads, preferred_element_type=jnp.float32) * scale
    allowed = (seg_rows[:, None] == seg_cols[None, :]) & (col_pos[None, :] <= row_pos[:, None])
    return jnp.where(allowed[None], scores, NEG_BIG)


def attention_forward(q_heads, k_heads, v_heads, seg_ids):
    head_count = q_heads.shape[0]
    row_total = q_heads.shape[1]
    block_rows = min(row_total, BLOCK_ROWS)
    block_count = row_total // block_rows
    col_pos = jnp.arange(row_total, dtype=jnp.int32)

    def one_block(start):
        row_pos = start + jnp.arange(block_rows, dtype=jnp.int32)
        scores = masked_scores(q_heads, k_heads, seg_ids, seg_ids, row_pos, col_pos)
        top_score = jnp.max(scores, axis=-1, keepdims=True)
        log_total = top_score + jnp.log(
            jnp.sum(jnp.exp(scores - top_score), axis=-1, keepdims=True)
        )
        prob_low = jnp.exp(scores - log_total).astype(jnp.bfloat16)
        attended = jnp.einsum("hqk,hkd->hqd", prob_low, v_heads, preferred_element_type=jnp.float32)
        return (attended.astype(jnp.bfloat16), log_total)

    starts = jnp.arange(block_count, dtype=jnp.int32) * block_rows
    attended, log_total = lax.map(one_block, starts)
    attended = attended.transpose(1, 0, 2, 3).reshape(head_count, row_total, -1)
    log_total = log_total.transpose(1, 0, 2, 3).reshape(head_count, row_total, 1)
    return (attended, log_total)


def attention_backward(q_heads, k_heads, v_heads, grad_att, log_total, seg_ids):
    scale = (DH + DR) ** (-0.5)
    head_count = q_heads.shape[0]
    row_total = q_heads.shape[1]
    block_rows = min(row_total, BLOCK_ROWS)
    block_count = row_total // block_rows
    col_pos = jnp.arange(row_total, dtype=jnp.int32)

    def one_block(carry, start):
        grad_k_acc, grad_v_acc = carry
        row_pos = start + jnp.arange(block_rows, dtype=jnp.int32)
        scores = masked_scores(q_heads, k_heads, seg_ids, seg_ids, row_pos, col_pos)
        prob_full = jnp.exp(scores - log_total)
        prob_low = prob_full.astype(jnp.bfloat16)
        grad_v_blk = jnp.einsum(
            "hqk,hqd->hkd", prob_low, grad_att, preferred_element_type=jnp.float32
        )
        grad_prob = jnp.einsum(
            "hqd,hkd->hqk", grad_att, v_heads, preferred_element_type=jnp.float32
        )
        row_dot = jnp.sum(prob_full * grad_prob, axis=-1, keepdims=True)
        grad_scores = (prob_full * (grad_prob - row_dot) * scale).astype(jnp.bfloat16)
        grad_q_blk = jnp.einsum(
            "hqk,hkc->hqc", grad_scores, k_heads, preferred_element_type=jnp.float32
        )
        grad_k_blk = jnp.einsum(
            "hqk,hqc->hkc", grad_scores, q_heads, preferred_element_type=jnp.float32
        )
        return ((grad_k_acc + grad_k_blk, grad_v_acc + grad_v_blk), grad_q_blk)

    starts = jnp.arange(block_count, dtype=jnp.int32) * block_rows
    init_acc = (jnp.zeros(k_heads.shape, jnp.float32), jnp.zeros(v_heads.shape, jnp.float32))
    (grad_k, grad_v), grad_q_blocks = lax.scan(one_block, init_acc, starts)
    grad_q = grad_q_blocks.transpose(1, 0, 2, 3).reshape(head_count, row_total, -1)
    return (grad_q, grad_k, grad_v)


MESH_IDS = pl.DeviceIdType.MESH
LOW = jnp.bfloat16
NT = (((1,), (1,)), ((), ()))
TN = (((0,), (0,)), ((), ()))


def axis_parts(mesh):
    devices = mesh.devices
    found = []
    for axis in range(devices.ndim):
        first = (0,) * devices.ndim
        line = [devices[first[:axis] + (i,) + first[axis + 1 :]] for i in range(devices.shape[axis])]
        places = [(*dev.coords, dev.core_on_chip) for dev in line]
        parts = []
        for k, name in enumerate(("x", "y", "z", "core")):
            values = [p[k] for p in places]
            if len(set(values)) > 1:
                stride = next(i for i, v in enumerate(values) if v != values[0])
                parts.append((stride, name, len(set(values))))
        found.append(tuple((name, size) for stride, name, size in sorted(parts, reverse=True)))
    return tuple(found)


def fits_kernels(mesh):
    wide, narrow = axis_parts(mesh)
    return (
        len(wide) == 2
        and wide[1][1] == 2
        and len(narrow) == 2
        and narrow[0][1] == 2
        and narrow[1] == ("core", 2)
    )


class Spot:
    def __init__(self, line):
        wide, narrow = lax.axis_index("wide"), lax.axis_index("narrow")
        self.line = line
        self.z, self.x = wide // 2, wide % 2
        self.y, self.c = narrow // 2, narrow % 2

    def wide(self, z, xf=0):
        return z * 2 + self.x + xf * (1 - 2 * self.x)

    def narrow(self, yf=0, cf=0):
        return (self.y + yf * (1 - 2 * self.y)) * 2 + self.c + cf * (1 - 2 * self.c)

    def device(self, z, xf=0, yf=0, cf=0):
        return {"wide": self.wide(z, xf), "narrow": self.narrow(yf, cf)}

    def flips(self, a, b, c):
        return a * (1 - c) + b * c, b * (1 - c) + a * c

    def index(self, z, a, b, cf=0):
        xf, yf = self.flips(a, b, self.c + cf * (1 - 2 * self.c))
        return self.wide(z, xf) * 4 + self.narrow(yf, cf)

    def routed(self, z, a, b):
        xf, yf = self.flips(a, b, self.c)
        return self.device(z, xf, yf)

    def inside(self, z):
        return (z >= 0) & (z < self.line)

    def near(self, rank):
        table = [sorted(range(self.line), key=lambda to: (abs(to - at), to))[rank] for at in range(self.line)]
        found = jnp.int32(table[0])
        for at in range(1, self.line):
            found = jnp.where(self.z == at, table[at], found)
        return found


def enter(spot, line_too, flips, wide_count=0):
    barrier = pltpu.get_barrier_semaphore()
    devices = [spot.device(spot.z, *flip) for flip in flips]
    if wide_count:
        here = spot.wide(spot.z)
        devices += [
            {"wide": lax.rem(here + step, wide_count), "narrow": spot.narrow()} for step in range(1, wide_count)
        ]
        devices = [dev for flip, dev in zip(flips, devices) if flip != (1, 0, 0)] + devices[len(flips) :]
        line_too = False
    for dev in devices:
        pl.semaphore_signal(barrier, inc=1, device_id=dev, device_id_type=MESH_IDS)
    if not line_too:
        pl.semaphore_wait(barrier, len(devices))
        return
    for step in (-1, 1):
        @pl.when(spot.inside(spot.z + step))
        def _():
            pl.semaphore_signal(barrier, inc=1, device_id=spot.device(spot.z + step), device_id_type=MESH_IDS)
    inner = spot.inside(spot.z - 1) & spot.inside(spot.z + 1)
    @pl.when(inner)
    def _():
        pl.semaphore_wait(barrier, len(devices) + 2)
    @pl.when(jnp.logical_not(inner))
    def _():
        pl.semaphore_wait(barrier, len(devices) + 1)


class Flow:
    def __init__(self, spot, kind, own, place, send, recv):
        self.spot, self.kind, self.own, self.place, self.send, self.recv = spot, kind, own, place, send, recv
        self.sent = []

    @staticmethod
    def steps(kind, line):
        ranks = (0,) if kind == "narrow" else range(line)
        firsts = (0,) if kind == "narrow" else (0, 1)
        seconds = (0,) if kind == "wide" else (0, 1)
        steps = [(r, a, b) for r in ranks for a in firsts for b in seconds]
        return sorted(steps, key=lambda s: (s[0] + s[1] + 2 * s[2], s[1], s[2]))

    @staticmethod
    def sends(kind, rank, a, b):
        moves = []
        if not a and not b and kind != "narrow":
            moves += ["up", "down"]
        if kind != "narrow" and not a and not b:
            moves.append("a")
        if kind != "wide" and not b:
            moves.append("b")
        if kind != "wide":
            moves.append("core")
        return moves

    @classmethod
    def send_count(cls, kind, line):
        return sum(len(cls.sends(kind, *step)) for step in cls.steps(kind, line))

    @staticmethod
    def blocks(kind, line):
        return {"all": line * 8, "wide": line * 2, "narrow": 4}[kind]

    def block(self, z, a, b, cf=0):
        if self.kind == "all":
            return self.spot.index(z, a, b, cf)
        return self.spot.wide(z, a) if self.kind == "wide" else self.spot.narrow(b, cf)

    def target(self, move):
        spot = self.spot
        if move in ("up", "down"):
            return spot.device(spot.z + (1 if move == "up" else -1))
        if move == "core":
            return spot.device(spot.z, 0, 0, 1)
        if self.kind == "all":
            return spot.routed(spot.z, int(move == "a"), int(move == "b"))
        return spot.device(spot.z, int(move == "a"), int(move == "b"))

    def copy(self, block, move, number, first=False):
        view = self.place(block)
        return pltpu.make_async_remote_copy(
            src_ref=self.own if first else view,
            dst_ref=view,
            send_sem=self.send.at[number],
            recv_sem=self.recv.at[block],
            device_id=self.target(move),
            device_id_type=MESH_IDS,
        )

    def arrive(self, block):
        self.copy(block, "a" if self.kind == "wide" else "core", 0).wait_recv()

    def step(self, rank, a, b):
        spot = self.spot
        z = spot.z if rank == 0 else spot.near(rank)
        block = self.block(z, a, b)
        first = rank == 0 and not a and not b
        if not first:
            self.arrive(block)
        for move in self.sends(self.kind, rank, a, b):
            copy = self.copy(block, move, len(self.sent), first)
            when = None
            if move == "up":
                when = spot.inside(spot.z + 1) & (z <= spot.z)
            elif move == "down":
                when = spot.inside(spot.z - 1) & (z >= spot.z)
            if when is None:
                copy.start()
            else:
                pl.when(when)(copy.start)
            self.sent.append((when, copy))

    def from_core(self, z, a, b):
        self.arrive(self.block(z, a, b, 1))

    def finish(self):
        for when, copy in self.sent:
            if when is None:
                copy.wait_send()
            else:
                pl.when(when)(copy.wait_send)


def move_kernel(line, items, *refs):
    count = len(items)
    srcs, dsts = refs[:count], refs[count : 2 * count]
    sends, recvs, local = refs[2 * count : 3 * count], refs[3 * count : 4 * count], refs[4 * count]
    spot = Spot(line)
    kinds = [item["kind"] for item in items]
    flips = set()
    for kind in kinds:
        flips |= {
            "all": {(1, 0, 0), (0, 1, 0), (0, 0, 1)},
            "wide": {(1, 0, 0)},
            "narrow": {(0, 1, 0), (0, 0, 1)},
            "wswap": set(),
            "nswap": {(0, 1, 0), (0, 0, 1), (0, 1, 1)},
        }[kind]
    wide_count = line * 2
    swaps = any(kind == "wswap" for kind in kinds)
    enter(spot, any(k in ("all", "wide") for k in kinds), sorted(flips), wide_count if swaps else 0)
    here_wide, here_narrow = spot.wide(spot.z), spot.narrow()

    flows, copies, own = [], [], []
    for i, item in enumerate(items):
        put = functools.partial(item["put"], dsts[i])
        if item["kind"] in ("wswap", "nswap"):
            continue
        flow = Flow(spot, item["kind"], srcs[i], put, sends[i], recvs[i])
        flows.append(flow)
        own.append(pltpu.make_async_copy(srcs[i], put(flow.block(spot.z, 0, 0)), local.at[i]))
    steps = sorted(
        ((step, flow) for flow in flows for step in Flow.steps(flow.kind, line)),
        key=lambda s: s[0][0] + s[0][1] + 2 * s[0][2],
    )
    for step, flow in steps:
        if step == (0, 0, 0):
            flow.step(*step)
    for i, item in enumerate(items):
        if item["kind"] == "wswap":
            peers = [(lax.rem(here_wide + k, wide_count), k) for k in range(1, wide_count)]
            for to, k in peers:
                copies.append((
                    pltpu.make_async_remote_copy(
                        src_ref=item["take"](srcs[i], to), dst_ref=item["put"](dsts[i], here_wide),
                        send_sem=sends[i].at[k], recv_sem=recvs[i].at[here_wide],
                        device_id={"wide": to, "narrow": here_narrow}, device_id_type=MESH_IDS,
                    ),
                    pltpu.make_async_remote_copy(
                        src_ref=item["take"](srcs[i], to), dst_ref=item["put"](dsts[i], to),
                        send_sem=sends[i].at[k], recv_sem=recvs[i].at[to],
                        device_id={"wide": to, "narrow": here_narrow}, device_id_type=MESH_IDS,
                    ),
                ))
            own.append(pltpu.make_async_copy(
                item["take"](srcs[i], here_wide), item["put"](dsts[i], here_wide), local.at[i]))
        elif item["kind"] == "nswap":
            for k, (yf, cf) in enumerate(((0, 1), (1, 0), (1, 1))):
                to = spot.narrow(yf, cf)
                dev = spot.device(spot.z, 0, yf, cf)
                copies.append((
                    pltpu.make_async_remote_copy(
                        src_ref=item["take"](srcs[i], to), dst_ref=item["put"](dsts[i], here_narrow),
                        send_sem=sends[i].at[k], recv_sem=recvs[i].at[here_narrow],
                        device_id=dev, device_id_type=MESH_IDS,
                    ),
                    pltpu.make_async_remote_copy(
                        src_ref=item["take"](srcs[i], to), dst_ref=item["put"](dsts[i], to),
                        send_sem=sends[i].at[k], recv_sem=recvs[i].at[to],
                        device_id=dev, device_id_type=MESH_IDS,
                    ),
                ))
            own.append(pltpu.make_async_copy(
                item["take"](srcs[i], here_narrow), item["put"](dsts[i], here_narrow), local.at[i]))
    for out, _ in copies:
        out.start()
    for copy in own:
        copy.start()
    for step, flow in steps:
        if step != (0, 0, 0):
            flow.step(*step)
    for flow in flows:
        if flow.kind != "wide":
            for rank, a, b in Flow.steps(flow.kind, line):
                flow.from_core(spot.z if rank == 0 else spot.near(rank), a, b)
    for _, back in copies:
        back.wait_recv()
    for flow in flows:
        flow.finish()
    for out, _ in copies:
        out.wait_send()
    for copy in own:
        copy.wait()


def move(line, items, collective_id):
    counts = {"all": line * 8, "wide": line * 2, "narrow": 4, "wswap": line * 2, "nswap": 4}
    dma = pltpu.SemaphoreType.DMA
    kinds = [item["kind"] for item in items]
    sends = [counts[kind] if kind in ("wswap", "nswap") else Flow.send_count(kind, line) for kind in kinds]
    moved = sum(item["array"].size * item["array"].dtype.itemsize * counts[item["kind"]] for item in items)
    return pl.pallas_call(
        functools.partial(move_kernel, line, items),
        out_shape=[jax.ShapeDtypeStruct(item["shape"], item["array"].dtype) for item in items],
        in_specs=[pl.BlockSpec(memory_space=pltpu.VMEM)] * len(items),
        out_specs=[pl.BlockSpec(memory_space=pl.ANY)] * len(items),
        scratch_shapes=[dma((n,)) for n in sends] + [dma((counts[kind],)) for kind in kinds] + [dma((len(items),))],
        compiler_params=pltpu.CompilerParams(collective_id=collective_id, has_side_effects=True),
        cost_estimate=pl.CostEstimate(flops=0, bytes_accessed=moved, transcendentals=0),
        name="move_blocks",
    )(*[item["array"] for item in items])


def narrow_sum_kernel(line, rows, part, out, held, summed, from_core, from_y,
                      load_sem, core_send, core_recv, y_send, y_recv):
    spot = Spot(line)
    enter(spot, False, [(0, 0, 1), (0, 1, 0)])

    def block(yf, cf):
        return part.at[pl.ds(pl.multiple_of(spot.narrow(yf, cf) * rows, rows), rows), :]

    def to_core(yf):
        return pltpu.make_async_remote_copy(
            src_ref=block(yf, 1), dst_ref=from_core.at[yf], send_sem=core_send.at[yf], recv_sem=core_recv.at[yf],
            device_id=spot.device(spot.z, 0, 0, 1), device_id_type=MESH_IDS,
        )

    def load(yf):
        return pltpu.make_async_copy(block(yf, 0), held.at[yf], load_sem.at[yf])

    over_y = pltpu.make_async_remote_copy(
        src_ref=summed, dst_ref=from_y, send_sem=y_send, recv_sem=y_recv,
        device_id=spot.device(spot.z, 0, 1, 0), device_id_type=MESH_IDS,
    )
    for yf in (1, 0):
        to_core(yf).start()
        load(yf).start()
    load(1).wait()
    to_core(1).wait_recv()
    summed[...] = (held[1].astype(jnp.float32) + from_core[1].astype(jnp.float32)).astype(summed.dtype)
    over_y.start()
    load(0).wait()
    to_core(0).wait_recv()
    total = held[0].astype(jnp.float32) + from_core[0].astype(jnp.float32)
    over_y.wait_recv()
    out[...] = total + from_y[...].astype(jnp.float32)
    over_y.wait_send()
    for yf in (1, 0):
        to_core(yf).wait_send()


def narrow_sum(line, part, collective_id):
    rows, width = part.shape[0] // 4, part.shape[1]
    dma = pltpu.SemaphoreType.DMA
    return pl.pallas_call(
        functools.partial(narrow_sum_kernel, line, rows),
        out_shape=jax.ShapeDtypeStruct((rows, width), jnp.float32),
        in_specs=[pl.BlockSpec(memory_space=pl.ANY)],
        out_specs=pl.BlockSpec(memory_space=pltpu.VMEM),
        scratch_shapes=[
            pltpu.VMEM((2, rows, width), part.dtype),
            pltpu.VMEM((rows, width), part.dtype),
            pltpu.VMEM((2, rows, width), part.dtype),
            pltpu.VMEM((rows, width), part.dtype),
            dma((2,)),
            dma((2,)),
            dma((2,)),
            dma,
            dma,
        ],
        compiler_params=pltpu.CompilerParams(collective_id=collective_id, has_side_effects=True),
        cost_estimate=pl.CostEstimate(
            flops=part.size, bytes_accessed=2 * part.size * part.dtype.itemsize, transcendentals=0
        ),
        name="narrow_sum",
    )(part)


def rows_in_kernel(line, sizes, hid_own, grad_own, gates, w_up, s_up, w_down, s_down,
                   hid_all, grad_all, act_e, act_s, dgu_e, dgu_s,
                   land_h, land_g, v_up, v_sup, v_down, v_sdown, t_act, t_sact, t_dgu, t_sdgu,
                   in_sem, h_send, h_recv, g_send, g_recv, own_sem, keep_sem, out_sem):
    rows, experts, hid, shared = sizes
    group = 4 * rows
    spot = Spot(line)
    loads = [
        pltpu.make_async_copy(src, dst, in_sem.at[i])
        for i, (src, dst) in enumerate(((w_up, v_up), (w_down, v_down), (s_up, v_sup), (s_down, v_sdown)))
    ]
    for copy in loads:
        copy.start()
    enter(spot, True, [(0, 0, 1), (0, 1, 0), (1, 0, 0)])

    def place(land, block):
        return land.at[pl.ds(pl.multiple_of(block * rows, rows), rows), :]

    flows = [
        Flow(spot, "all", hid_own, functools.partial(place, land_h), h_send, h_recv),
        Flow(spot, "all", grad_own, functools.partial(place, land_g), g_send, g_recv),
    ]
    for flow in flows:
        flow.step(0, 0, 0)
    mine = flows[0].block(spot.z, 0, 0)
    own = [
        pltpu.make_async_copy(hid_own, place(land_h, mine), own_sem.at[0]),
        pltpu.make_async_copy(grad_own, place(land_g, mine), own_sem.at[1]),
    ]
    for copy in own:
        copy.start()

    def keeps(n, at):
        span = pl.ds(pl.multiple_of(at * group, group), group)
        return (
            pltpu.make_async_copy(land_h.at[span, :], hid_all.at[span, :], keep_sem.at[0, n]),
            pltpu.make_async_copy(land_g.at[span, :], grad_all.at[span, :], keep_sem.at[1, n]),
        )

    def stores(n, at):
        cols = pl.ds(pl.multiple_of(at * group, group), group)
        slot = n % 2
        pairs = (
            (t_act.at[slot], act_e.at[:, cols], out_sem.at[0, slot]),
            (t_sact.at[slot], act_s.at[:, cols], out_sem.at[1, slot]),
            (t_dgu.at[slot], dgu_e.at[:, cols], out_sem.at[2, slot]),
            (t_sdgu.at[slot], dgu_s.at[:, cols], out_sem.at[3, slot]),
        )
        return [pltpu.make_async_copy(*pair) for pair in pairs]

    def both_ways(gate_part, up_part, grad_part, gate):
        sig = 1.0 / (1.0 + jnp.exp(-gate_part))
        silu = gate_part * sig
        if gate is not None:
            grad_part = grad_part * gate
        grad_gate = grad_part * up_part * (sig + silu * (1.0 - sig))
        act = silu * up_part
        if gate is not None:
            act = act * gate
        return act.astype(LOW), grad_gate.astype(LOW), (grad_part * silu).astype(LOW)

    done = []

    def compute(at):
        n = len(done)
        if n >= 2:
            for copy in stores(n - 2, done[n - 2]):
                copy.wait()
        slot = n % 2
        cols = pl.ds(pl.multiple_of(at * group, group), group)
        h, g = land_h[cols, :], land_g[cols, :]
        for e in range(experts):
            gu = lax.dot_general(
                v_up[2 * e * hid : 2 * (e + 1) * hid, :], h, NT, preferred_element_type=jnp.float32
            )
            da = lax.dot_general(v_down[e * hid : (e + 1) * hid, :], g, NT, preferred_element_type=jnp.float32)
            act, dg, du = both_ways(gu[:hid], gu[hid:], da, gates[e : e + 1, cols])
            t_act[slot, e * hid : (e + 1) * hid, :] = act
            t_dgu[slot, 2 * e * hid : (2 * e + 1) * hid, :] = dg
            t_dgu[slot, (2 * e + 1) * hid : 2 * (e + 1) * hid, :] = du
        gu = lax.dot_general(v_sup[...], h, NT, preferred_element_type=jnp.float32)
        da = lax.dot_general(v_sdown[...], g, NT, preferred_element_type=jnp.float32)
        act, dg, du = both_ways(gu[:shared], gu[shared:], da, None)
        t_sact[slot] = act
        t_sdgu[slot, :shared, :] = dg
        t_sdgu[slot, shared:, :] = du
        done.append(at)
        for copy in (*keeps(n, at), *stores(n, at)):
            copy.start()

    waiting = sorted(
        ((s[0] + s[1] + 2 * s[2], s) for s in Flow.steps("all", line) if s != (0, 0, 0)), key=lambda s: s[0]
    )
    loaded = False
    for _, (rank, a, b) in waiting:
        for flow in flows:
            flow.step(rank, a, b)
        if a and b:
            z = spot.z if rank == 0 else spot.near(rank)
            if not loaded:
                loaded = True
                for copy in own + loads:
                    copy.wait()
            for xf in (0, 1):
                for flow in flows:
                    for other in (0, 1):
                        ca = xf * spot.c + other * (1 - spot.c)
                        cb = other * spot.c + xf * (1 - spot.c)
                        flow.from_core(z, ca, cb)
                compute(spot.wide(z, xf))
    for flow in flows:
        flow.finish()
    count = len(done)
    for n, at in enumerate(done):
        for copy in (*keeps(n, at), *(stores(n, at) if n >= count - 2 else ())):
            copy.wait()


def rows_in(line, hid_own, grad_own, gates, w_up, s_up, w_down, s_down, experts, collective_id):
    rows, width = hid_own.shape
    tokens = rows * line * 8
    hid, shared = w_down.shape[0] // experts, s_down.shape[0]
    group = 4 * rows
    dma = pltpu.SemaphoreType.DMA
    hbm = pl.BlockSpec(memory_space=pl.ANY)
    vmem = pl.BlockSpec(memory_space=pltpu.VMEM)
    sends = Flow.send_count("all", line)
    out = [(tokens, width), (tokens, width)]
    out += [(f, tokens) for f in (w_down.shape[0], shared, w_up.shape[0], 2 * shared)]
    return pl.pallas_call(
        functools.partial(rows_in_kernel, line, (rows, experts, hid, shared)),
        out_shape=[jax.ShapeDtypeStruct(shape, LOW) for shape in out],
        in_specs=[vmem, vmem, vmem] + [hbm] * 4,
        out_specs=[hbm] * 6,
        scratch_shapes=[pltpu.VMEM((tokens, width), LOW)] * 2
        + [pltpu.VMEM(arr.shape, LOW) for arr in (w_up, s_up, w_down, s_down)]
        + [pltpu.VMEM((2, f, group), LOW) for f in (w_down.shape[0], shared, w_up.shape[0], 2 * shared)]
        + [
            dma((4,)),
            dma((sends,)),
            dma((line * 8,)),
            dma((sends,)),
            dma((line * 8,)),
            dma((2,)),
            dma((2, line * 2)),
            dma((4, 2)),
        ],
        compiler_params=pltpu.CompilerParams(
            collective_id=collective_id, has_side_effects=True, vmem_limit_bytes=60 << 20
        ),
        cost_estimate=pl.CostEstimate(
            flops=6 * (w_down.shape[0] + shared) * tokens * width,
            bytes_accessed=6 * tokens * width,
            transcendentals=(w_down.shape[0] + shared) * tokens,
        ),
        name="rows_in",
    )(hid_own, grad_own, gates, w_up, s_up, w_down, s_down)


class Sum:
    def __init__(self, spot, rows, lhs, w, loads, refs):
        self.spot, self.rows, self.lhs, self.w, self.loads = spot, rows, lhs, w, loads
        (self.stage, self.core_buf, self.b_buf, self.a_buf, self.z_buf,
         self.core_send, self.core_recv, self.b_send, self.b_recv, self.a_send, self.a_recv,
         self.z_send, self.z_recv) = refs

    def zed(self, j):
        rank = self.spot.line - 1 - j
        return self.spot.z if rank == 0 else self.spot.near(rank)

    def group(self, xf, j):
        z = self.zed(j)
        return z, self.spot.wide(z, xf)

    def place(self, at, yf, cf):
        start = pl.multiple_of(self.spot.narrow(yf, cf) * self.rows, self.rows)
        return self.stage.at[at, pl.ds(start, self.rows), :]

    def copy(self, src, dst, send, recv, number, to, device):
        return pltpu.make_async_remote_copy(
            src_ref=src, dst_ref=dst.at[to], send_sem=send.at[number], recv_sem=recv.at[to],
            device_id=device, device_id_type=MESH_IDS,
        )

    def to_core(self, z, at, xf, yf):
        s = (z * 2 + xf) * 2 + yf
        return self.copy(self.place(at, yf, 1), self.core_buf, self.core_send, self.core_recv, s, s,
                         self.spot.device(self.spot.z, 0, 0, 1))

    def to_b(self, z, at, yf, a):
        s = z * 2 + a
        return self.copy(self.place(at, yf, 0), self.b_buf, self.b_send, self.b_recv, s, s,
                         self.spot.routed(self.spot.z, 0, 1))

    def to_a(self, z, at, yf):
        return self.copy(self.place(at, yf, 0), self.a_buf, self.a_send, self.a_recv, z, z,
                         self.spot.routed(self.spot.z, 1, 0))

    def to_z(self, z, at, down):
        return self.copy(self.place(at, 0, 0), self.z_buf, self.z_send, self.z_recv, z, down * self.spot.line + z,
                         self.spot.device(self.spot.z + 1 - 2 * down))

    def only(self, core, act):
        pl.when(self.spot.c == core)(act)

    def produce(self, xf, j, chunk):
        z, at = self.group(xf, j)
        size = 4 * self.rows
        cols = pl.ds(pl.multiple_of(at * size, size), size)
        for copy in self.loads(xf, j, at):
            copy.wait()
        width = self.stage.shape[2]

        @pl.loop(0, width // chunk)
        def _(t):
            cut = pl.ds(pl.multiple_of(t * chunk, chunk), chunk)
            value = sum(
                lax.dot_general(lhs[:, cols], w[:, cut], TN, preferred_element_type=jnp.float32)
                for lhs, w in zip(self.lhs, self.w)
            )
            self.stage[at, :, cut] = value.astype(LOW)

        for yf in (1, 0):
            self.to_core(z, at, xf, yf).start()

    def joined(self, z, at, xf, yf):
        self.to_core(z, at, xf, yf).wait_recv()
        there = self.core_buf[(z * 2 + xf) * 2 + yf]
        return self.place(at, yf, 0)[...].astype(jnp.float32) + there.astype(jnp.float32)

    def send_b(self, xf, yf, a, j):
        z, at = self.group(xf, j)
        self.place(at, yf, 0)[...] = self.joined(z, at, xf, yf).astype(LOW)
        self.to_b(z, at, yf, a).start()

    def send_a(self, xf, yf, j):
        z, at = self.group(xf, j)
        value = self.joined(z, at, xf, yf)
        self.to_b(z, at, yf, 1).wait_recv()
        self.place(at, yf, 0)[...] = (value + self.b_buf[z * 2 + 1].astype(jnp.float32)).astype(LOW)
        self.to_a(z, at, yf).start()

    def send_z(self, j, out):
        spot = self.spot
        z, at = self.group(0, j)
        value = self.joined(z, at, 0, 0)
        self.to_b(z, at, 0, 0).wait_recv()
        self.to_a(z, at, 0).wait_recv()
        value += self.b_buf[z * 2].astype(jnp.float32) + self.a_buf[z].astype(jnp.float32)
        last = j == spot.line - 1
        if last:
            out[...] = value
        else:
            self.place(at, 0, 0)[...] = value.astype(LOW)
        for down in (0, 1):
            behind = spot.inside(spot.z - 1 + 2 * down)
            if last:
                @pl.when(behind)
                def _():
                    self.to_z(z, at, down).wait_recv()
                    out[...] += self.z_buf[down * spot.line + z].astype(jnp.float32)
            else:
                @pl.when((z < spot.z) if down else (z > spot.z))
                def _():
                    @pl.when(behind)
                    def _():
                        self.to_z(z, at, down).wait_recv()
                        more = self.place(at, 0, 0)[...].astype(jnp.float32)
                        more += self.z_buf[down * spot.line + z].astype(jnp.float32)
                        self.place(at, 0, 0)[...] = more.astype(LOW)
                    self.to_z(z, at, down).start()

    def early(self, j):
        self.send_b(1, 1, 1, j)
        self.only(1, lambda: self.send_b(1, 0, 0, j))

    def middle(self, j):
        self.only(0, lambda: self.send_b(0, 1, 0, j))
        self.only(0, lambda: self.send_a(1, 0, j))

    def late(self, j):
        self.only(1, lambda: self.send_a(0, 1, j))

    def finish(self):
        for j in range(self.spot.line):
            for xf in (1, 0):
                z, at = self.group(xf, j)
                for yf in (1, 0):
                    self.to_core(z, at, xf, yf).wait_send()
            z, at = self.group(1, j)
            self.to_b(z, at, 1, 1).wait_send()
            self.only(1, lambda: self.to_b(z, at, 0, 0).wait_send())
            self.only(0, lambda: self.to_a(z, at, 0).wait_send())
            z2, at2 = self.group(0, j)
            self.only(0, lambda: self.to_b(z2, at2, 1, 0).wait_send())
            self.only(1, lambda: self.to_a(z2, at2, 1).wait_send())
            if j < self.spot.line - 1:
                for down in (0, 1):
                    @pl.when((z2 < self.spot.z) if down else (z2 > self.spot.z))
                    def _():
                        self.to_z(z2, at2, down).wait_send()


def rows_out_kernel(line, rows, chunk, count, *refs):
    spot = Spot(line)
    lefts, rights = refs[: 2 * count], refs[2 * count : 4 * count]
    outs = refs[4 * count : 5 * count]
    v_lefts, v_rights = refs[5 * count : 7 * count], refs[7 * count : 9 * count]
    rest = refs[9 * count :]
    in_sem, lhs_sem = rest[:2]
    per = 13
    size = 4 * rows
    right_loads = [pltpu.make_async_copy(rights[k], v_rights[k], in_sem.at[k]) for k in range(2 * count)]

    def loader(s):
        def loads(xf, j, at):
            cols = pl.ds(pl.multiple_of(at * size, size), size)
            return [
                pltpu.make_async_copy(
                    lefts[k].at[:, cols], v_lefts[k].at[:, cols], lhs_sem.at[k, (1 - xf) * line + j]
                )
                for k in (2 * s, 2 * s + 1)
            ]

        return loads

    sums = [
        Sum(spot, rows, v_lefts[2 * s : 2 * s + 2], v_rights[2 * s : 2 * s + 2], loader(s),
            rest[2 + s * per : 2 + (s + 1) * per])
        for s in range(count)
    ]
    for s, one in enumerate(sums):
        for k in (2 * s, 2 * s + 1):
            right_loads[k].start()
        for xf in (1, 0):
            for j in range(line):
                _, at = one.group(xf, j)
                for copy in one.loads(xf, j, at):
                    copy.start()
    enter(spot, True, [(0, 0, 1), (0, 1, 0), (1, 0, 0)])
    ready = set()

    def produce(s, xf, j):
        if s not in ready:
            ready.add(s)
            for k in (2 * s, 2 * s + 1):
                right_loads[k].wait()
        sums[s].produce(xf, j, chunk)

    first = sums[0]
    for j in range(line):
        produce(0, 1, j)
        if j:
            first.early(j - 1)
    for j in range(line):
        produce(0, 0, j)
        if j == 0:
            first.early(line - 1)
        else:
            first.middle(j - 1)
    for s in range(1, count):
        later = sums[s]
        produce(s, 1, 0)
        if s == 1:
            first.middle(line - 1)
        for j in range(1, line):
            produce(s, 1, j)
            later.early(j - 1)
            if s == 1:
                first.late(j - 1)
        produce(s, 0, 0)
        later.early(line - 1)
        if s == 1:
            first.late(line - 1)
        for j in range(1, line):
            produce(s, 0, j)
            later.middle(j - 1)
            if s == 1:
                first.send_z(j - 1, outs[0])
        if s == 1:
            first.send_z(line - 1, outs[0])
        later.middle(line - 1)
        for j in range(line):
            later.late(j)
        for j in range(line):
            later.send_z(j, outs[s])
    if count == 1:
        first.middle(line - 1)
        for j in range(line):
            first.late(j)
        for j in range(line):
            first.send_z(j, outs[0])
    for one in sums:
        one.finish()


def rows_out(line, pairs, collective_id, chunk=512):
    count = len(pairs)
    lefts = [left for pair in pairs for left, _ in pair]
    rights = [right for pair in pairs for _, right in pair]
    tokens, width = lefts[0].shape[1], rights[0].shape[1]
    rows = tokens // (line * 8)
    dma = pltpu.SemaphoreType.DMA
    slots = line * 4
    scratch = [pltpu.VMEM(arr.shape, LOW) for arr in lefts + rights] + [dma((2 * count,)), dma((2 * count, line * 2))]
    for _ in range(count):
        scratch += [
            pltpu.VMEM((line * 2, 4 * rows, width), LOW),
            pltpu.VMEM((slots, rows, width), LOW),
            pltpu.VMEM((line * 2, rows, width), LOW),
            pltpu.VMEM((line, rows, width), LOW),
            pltpu.VMEM((line * 2, rows, width), LOW),
            dma((slots,)),
            dma((slots,)),
            dma((line * 2,)),
            dma((line * 2,)),
            dma((line,)),
            dma((line,)),
            dma((line,)),
            dma((line * 2,)),
        ]
    return pl.pallas_call(
        functools.partial(rows_out_kernel, line, rows, chunk, count),
        out_shape=[jax.ShapeDtypeStruct((rows, width), jnp.float32)] * count,
        in_specs=[pl.BlockSpec(memory_space=pl.ANY)] * (4 * count),
        out_specs=[pl.BlockSpec(memory_space=pltpu.VMEM)] * count,
        scratch_shapes=scratch,
        compiler_params=pltpu.CompilerParams(
            collective_id=collective_id, has_side_effects=True, vmem_limit_bytes=63 << 20
        ),
        cost_estimate=pl.CostEstimate(
            flops=2 * sum(arr.shape[0] for arr in lefts) * tokens * width,
            bytes_accessed=4 * count * tokens * width,
            transcendentals=0,
        ),
        name="rows_out",
    )(*lefts, *rights)

class Links:
    AXES = {"all": ("wide", "narrow"), "wide": "wide", "narrow": "narrow", "wswap": "wide", "nswap": "narrow"}

    def __init__(self, mesh):
        self.line = axis_parts(mesh)[0][0][1] if fits_kernels(mesh) else None
        self.shape = dict(mesh.shape)
        self.calls = 0

    def number(self):
        self.calls += 1
        return self.calls

    def item(self, array, kind, shape, put, take, plain):
        return {"array": array, "kind": kind, "shape": shape, "put": put, "take": take, "plain": plain}

    @staticmethod
    def part(axis, size):
        def view(ref, index):
            cut = pl.ds(pl.multiple_of(index * size, size), size)
            return ref.at[tuple(cut if k == axis else slice(None) for k in range(len(ref.shape)))]

        return view

    def count(self, kind):
        return self.shape["wide"] * self.shape["narrow"] if kind == "all" else self.shape[self.AXES[kind]]

    def gather(self, array, kind, axis):
        shape = list(array.shape)
        shape[axis] *= self.count(kind)
        plain = functools.partial(lax.all_gather, array, self.AXES[kind], axis=axis, tiled=True)
        return self.item(array, kind, tuple(shape), self.part(axis, array.shape[axis]), None, plain)

    def swap(self, array, kind, split, concat):
        count = self.count(kind)
        shape = list(array.shape)
        shape[split] //= count
        size = shape[split]
        put = self.part(concat, array.shape[concat])
        shape[concat] *= count
        plain = functools.partial(
            lax.all_to_all, array, self.AXES[kind], split_axis=split, concat_axis=concat, tiled=True
        )
        return self.item(array, kind, tuple(shape), put, self.part(split, size), plain)

    def grid(self, array):
        rows, cols = array.shape
        down, across = self.shape["narrow"], self.shape["wide"]

        def put(ref, index):
            at_row = pl.multiple_of((index % down) * rows, rows)
            at_col = pl.multiple_of((index // down) * cols, cols)
            return ref.at[pl.ds(at_row, rows), pl.ds(at_col, cols)]

        def plain():
            return lax.all_gather(lax.all_gather(array, "narrow", axis=0, tiled=True), "wide", axis=1, tiled=True)

        return self.item(array, "all", (rows * down, cols * across), put, None, plain)

    def weave(self, array):
        shape = (array.shape[0], self.shape["narrow"], *array.shape[1:])
        plain = functools.partial(lax.all_gather, array, "narrow", axis=1)
        return self.item(array, "narrow", shape, lambda ref, index: ref.at[:, index], None, plain)

    def move(self, *items):
        if self.line:
            return move(self.line, items, self.number())
        return [item["plain"]() for item in items]

    def narrow_sum(self, part):
        if self.line:
            return narrow_sum(self.line, part, self.number())
        return lax.psum_scatter(part, "narrow", scatter_dimension=0, tiled=True).astype(jnp.float32)

    def rows_in(self, hidden, grad, gates, w_up, s_up, w_down, s_down, experts):
        if self.line:
            return rows_in(self.line, hidden, grad, gates, w_up, s_up, w_down, s_down, experts, self.number())
        hidden, grad = (lax.all_gather(rows, self.AXES["all"], axis=0, tiled=True) for rows in (hidden, grad))

        def both_ways(up, down, gate):
            gu, grad_act = dot_nt(up, hidden), dot_nt(down, grad) * gate
            gate_part, up_part = jnp.split(gu, 2)
            sig = jax.nn.sigmoid(gate_part)
            grad_gate = grad_act * up_part * sig * (1.0 + gate_part * (1.0 - sig))
            grad_up = grad_act * gate_part * sig
            act = gate_part * sig * up_part * gate
            return act.astype(LOW), jnp.concatenate([grad_gate.astype(LOW), grad_up.astype(LOW)])

        ups, downs = jnp.split(w_up, experts), jnp.split(w_down, experts)
        pairs = [both_ways(ups[e], downs[e], gates[e : e + 1]) for e in range(experts)]
        act_s, dgu_s = both_ways(s_up, s_down, 1.0)
        acts, dgus = (jnp.concatenate(parts) for parts in zip(*pairs))
        return hidden, grad, acts, act_s, dgus, dgu_s

    def rows_out(self, *pairs):
        if self.line:
            return rows_out(self.line, pairs, self.number())
        sums = []
        for pair in pairs:
            term = sum(dot_tn(left, right) for left, right in pair).astype(LOW)
            term = lax.psum_scatter(term, self.AXES["all"], scatter_dimension=0, tiled=True)
            sums.append(term.astype(jnp.float32))
        return sums


def rows_of(array, index, count):
    return lax.dynamic_slice_in_dim(array, index * count, count, 0)


def dot_nt(lhs, rhs):
    return lax.dot_general(lhs, rhs, (((1,), (1,)), ((), ())), preferred_element_type=jnp.float32)


def dot_tn(lhs, rhs):
    return lax.dot_general(lhs, rhs, (((0,), (0,)), ((), ())), preferred_element_type=jnp.float32)


def dot_nn(lhs, rhs):
    return jnp.dot(lhs, rhs, preferred_element_type=jnp.float32)


def per_device(
    links,
    tokens_in,
    seg_ids,
    routes,
    gate_vals,
    attn_gain,
    w_query,
    w_latent,
    latent_gain,
    w_expand,
    w_output,
    ffn_gain,
    w_shared_in,
    w_shared_out,
    w_expert_in,
    w_expert_out,
    grad_output,
):
    links.calls = 0
    low = LOW
    wide_count = lax.axis_size("wide")
    narrow_count = lax.axis_size("narrow")
    wide_at = lax.axis_index("wide")
    narrow_at = lax.axis_index("narrow")
    tok_rows, width = tokens_in.shape
    own_rows = tok_rows // narrow_count
    local_experts, _, _, hidden_local = w_expert_in.shape
    num_experts = local_experts * wide_count
    head_local = w_query.shape[1] // (DH + DR)

    def mine(array):
        return rows_of(array, narrow_at, own_rows)

    x_float = tokens_in.astype(jnp.float32)
    x_normed, inv_one = rms_forward(x_float, attn_gain)
    x_low = x_normed.astype(low)
    latent_part = rows_of(w_latent.T, narrow_at, w_latent.shape[1] // narrow_count)
    chosen = routes[:, :, None] == jnp.arange(num_experts, dtype=jnp.int32)
    gate_table = jnp.sum(jnp.where(chosen, gate_vals[:, :, None], 0.0), axis=1).T
    gate_table = gate_table.reshape(wide_count, local_experts, tok_rows)
    gate_table = jnp.pad(gate_table, ((0, 0), (0, -local_experts % 8), (0, 0))).reshape(-1, tok_rows)
    wq_all, wkva_all, wkvb_all, wo_all, shared_in, shared_out, gates, x_part = links.move(
        links.gather(w_query, "wide", 0),
        links.grid(latent_part),
        links.gather(w_expand, "wide", 0),
        links.gather(w_output, "wide", 1),
        links.swap(w_shared_in.transpose(1, 2, 0), "wswap", 1, 2),
        links.swap(w_shared_out, "wswap", 0, 1),
        links.swap(gate_table, "wswap", 0, 1),
        links.swap(mine(x_low), "wswap", 1, 0),
    )

    cos_tab, sin_tab = rotary_tables(positions(seg_ids))
    queries = dot_nn(x_low, wq_all).reshape(tok_rows, head_local, DH + DR).transpose(1, 0, 2)
    q_heads = jnp.concatenate(
        [queries[..., :DH], rotate(queries[..., DH:], cos_tab, sin_tab)], -1
    ).astype(low)
    latent_all = dot_nt(x_low, wkva_all)
    latent = latent_all[:, :KVR]
    latent_normed, inv_lat = rms_forward(latent, latent_gain)
    latent_low = latent_normed.astype(low)
    key_rope = rotate(latent_all[:, KVR:], cos_tab, sin_tab).astype(low)
    expanded = dot_nn(latent_low, wkvb_all).reshape(tok_rows, head_local, 2 * DH).transpose(1, 0, 2)
    key_nope = expanded[..., :DH].astype(low)
    v_heads = expanded[..., DH:].astype(low)
    k_heads = jnp.concatenate(
        [key_nope, jnp.broadcast_to(key_rope[None], (head_local, tok_rows, DR))], -1
    )
    attended, log_total = attention_forward(q_heads, k_heads, v_heads, seg_ids)
    merged = attended.transpose(1, 0, 2).reshape(tok_rows, head_local * DH)
    mixed = links.narrow_sum(dot_nn(merged, wo_all).astype(low))

    x_rows = mine(x_float)
    inv_one_rows = mine(inv_one)
    resid = x_rows + mixed
    resid_normed, inv_two = rms_forward(resid, ffn_gain)

    expert_rows = local_experts * hidden_local
    w_up = w_expert_in.transpose(0, 2, 3, 1).reshape(2 * expert_rows, width)
    w_down = w_expert_out.reshape(expert_rows, width)
    s_up = shared_in.reshape(-1, width)
    hidden, grad_all, act_exp, act_sh, grad_gu_exp, grad_gu_sh = links.rows_in(
        resid_normed.astype(low), mine(grad_output), gates, w_up, s_up, w_down, shared_out, local_experts
    )
    grad_hidden, out_rows = links.rows_out(
        ((grad_gu_exp, w_up), (grad_gu_sh, s_up)), ((act_exp, w_down), (act_sh, shared_out))
    )
    grad_exp_out = dot_nn(act_exp, grad_all).reshape(local_experts, hidden_local, width)
    grad_shout = dot_nn(act_sh, grad_all).astype(low)
    grad_exp_in = dot_nn(grad_gu_exp, hidden).reshape(local_experts, 2, hidden_local, width)
    grad_exp_in = grad_exp_in.transpose(0, 3, 1, 2)
    grad_shin = dot_nn(grad_gu_sh, hidden).reshape(2, -1, width).astype(low)
    out_rows = (resid + out_rows).astype(low)

    grad_resid, grad_ffn = rms_backward(resid, inv_two, ffn_gain, grad_hidden)
    grad_resid = grad_resid + mine(grad_output).astype(jnp.float32)
    grad_low, x_cols = links.move(
        links.gather(grad_resid.astype(low), "narrow", 0),
        links.weave(x_part.reshape(wide_count, own_rows, -1)),
    )
    x_cols = x_cols.reshape(wide_count * tok_rows, -1)
    grad_merged = dot_nt(grad_low, wo_all)
    grad_wo = dot_tn(merged, grad_low).astype(low)
    red_wo = lax.psum_scatter(grad_wo, "wide", scatter_dimension=1, tiled=True)
    grad_att = grad_merged.reshape(tok_rows, head_local, DH).transpose(1, 0, 2).astype(low)
    grad_q, grad_k, grad_v = attention_backward(
        q_heads, k_heads, v_heads, grad_att, log_total, seg_ids
    )
    grad_q_pre = jnp.concatenate(
        [grad_q[..., :DH], unrotate(grad_q[..., DH:], cos_tab, sin_tab)], -1
    ).astype(low)
    grad_q_pre = grad_q_pre.transpose(1, 0, 2).reshape(tok_rows, head_local * (DH + DR))
    grad_rope_part = jnp.sum(grad_k[..., DH:], axis=0)
    grad_expanded = jnp.concatenate([grad_k[..., :DH], grad_v], -1).astype(low)
    grad_expanded = grad_expanded.transpose(1, 0, 2).reshape(tok_rows, head_local * 2 * DH)
    grad_wkvb = dot_tn(latent_low, grad_expanded).astype(low)
    red_wkvb = lax.psum_scatter(grad_wkvb, "wide", scatter_dimension=0, tiled=True)
    grad_latent_part = dot_nt(grad_expanded, wkvb_all)
    grad_x_part = dot_nt(grad_q_pre, wq_all)
    terms = jnp.concatenate([grad_x_part, grad_latent_part, grad_rope_part], 1)
    terms = links.narrow_sum(terms.astype(low))
    grad_x_query, latent_terms = terms[:, :width], terms[:, width:]
    grad_latent, grad_lat_gain = rms_backward(
        mine(latent), mine(inv_lat), latent_gain, latent_terms[:, :KVR]
    )
    grad_rope = unrotate(latent_terms[:, KVR:], mine(cos_tab), mine(sin_tab))
    grad_latent_all = jnp.concatenate([grad_latent, grad_rope], -1).astype(low)
    grad_x_normed = grad_x_query + dot_nn(grad_latent_all, wkva_all)
    grad_x, grad_att_gain = rms_backward(x_rows, inv_one_rows, attn_gain, grad_x_normed)
    grad_tokens = (grad_x + grad_resid).astype(low)
    gains = jnp.concatenate(
        [part.reshape(wide_count, -1) for part in (grad_att_gain, grad_ffn, grad_lat_gain)], 1
    )
    q_pre_all, latent_rows, grad_tokens, layer_out, red_shout, red_shin, gains = links.move(
        links.gather(grad_q_pre, "wide", 0),
        links.gather(grad_latent_all, "all", 0),
        links.gather(grad_tokens, "narrow", 0),
        links.swap(out_rows, "nswap", 1, 0),
        links.swap(grad_shout, "wswap", 1, 0),
        links.swap(grad_shin, "wswap", 2, 1),
        links.gather(gains, "all", 0),
    )
    red_wkva = dot_tn(x_cols, latent_rows)
    red_wq = dot_tn(x_cols, q_pre_all)
    gains = gains.reshape(-1, wide_count, gains.shape[1])
    gains = jnp.sum(lax.dynamic_index_in_dim(gains, wide_at, 1, keepdims=False), axis=0)
    part = width // wide_count
    red_att_gain, red_ffn, red_lat_gain = gains[:part], gains[part : 2 * part], gains[2 * part :]
    return (
        layer_out,
        grad_tokens.astype(jnp.float32),
        red_att_gain,
        red_wq,
        red_wkva,
        red_lat_gain,
        red_wkvb.astype(jnp.float32),
        red_wo.astype(jnp.float32),
        red_ffn,
        red_shin.astype(jnp.float32).transpose(2, 0, 1),
        red_shout.astype(jnp.float32),
        grad_exp_in,
        grad_exp_out,
    )


def solution(mesh):
    placed = (
        P("wide", None),
        P("wide"),
        P("wide", None),
        P("wide", None),
        P(),
        P("wide", "narrow"),
        P("wide", None),
        P(),
        P("wide", "narrow"),
        P("narrow", "wide"),
        P(),
        P("wide", None, "narrow"),
        P("narrow", "wide"),
        P("wide", None, None, "narrow"),
        P("wide", "narrow", None),
        P("wide", None),
    )
    return jax.shard_map(
        functools.partial(per_device, Links(mesh)),
        mesh=mesh,
        in_specs=placed,
        out_specs=(
            P("wide", "narrow"),
            P("wide", None),
            P("wide"),
            P("wide", "narrow"),
            P("wide", None),
            P("wide"),
            P("wide", "narrow"),
            P("narrow", "wide"),
            P("wide"),
            P("wide", None, "narrow"),
            P("narrow", "wide"),
            P("wide", None, None, "narrow"),
            P("wide", "narrow", None),
        ),
        check_vma=False,
    )
```

```python
import functools

import jax
import jax.numpy as jnp
from jax import lax
from jax.experimental import pallas as pl
from jax.experimental.pallas import tpu as pltpu
from jax.sharding import PartitionSpec as P

DH = 128
DR = 64
KVR = 512


EPS = 1e-06
THETA = 50000.0
NEG_BIG = -1e30
BLOCK_ROWS = 512


def positions(seg_ids):
    row_index = jnp.arange(seg_ids.shape[0], dtype=jnp.int32)
    starts = jnp.concatenate([jnp.ones((1,), dtype=bool), seg_ids[1:] != seg_ids[:-1]])
    begins = lax.cummax(jnp.where(starts, row_index, 0), axis=0)
    return (row_index - begins).astype(jnp.float32)


def rotary_tables(pos_float):
    half_dim = DR // 2
    inv_freq = THETA ** (-(jnp.arange(half_dim, dtype=jnp.float32) * 2.0 / DR))
    angles = pos_float[:, None] * inv_freq[None, :]
    return (jnp.cos(angles), jnp.sin(angles))


def rotate(values, cos_tab, sin_tab):
    half_dim = values.shape[-1] // 2
    lower_half = values[..., :half_dim]
    upper_half = values[..., half_dim:]
    return jnp.concatenate(
        [lower_half * cos_tab - upper_half * sin_tab, upper_half * cos_tab + lower_half * sin_tab],
        -1,
    )


def unrotate(values, cos_tab, sin_tab):
    half_dim = values.shape[-1] // 2
    lower_half = values[..., :half_dim]
    upper_half = values[..., half_dim:]
    return jnp.concatenate(
        [lower_half * cos_tab + upper_half * sin_tab, upper_half * cos_tab - lower_half * sin_tab],
        -1,
    )


def rms_forward(values, gain_vec):
    inv_rms = lax.rsqrt(jnp.mean(values * values, axis=-1, keepdims=True) + EPS)
    return (values * inv_rms * gain_vec, inv_rms)


def rms_backward(values, inv_rms, gain_vec, grad_out):
    scaled = grad_out * gain_vec
    grad_in = inv_rms * scaled - values * inv_rms**3 * jnp.mean(
        values * scaled, axis=-1, keepdims=True
    )
    grad_gain = jnp.sum(grad_out * values * inv_rms, axis=0)
    return (grad_in, grad_gain)


def masked_scores(q_blk, k_heads, seg_rows, seg_cols, row_pos, col_pos):
    scale = (DH + DR) ** (-0.5)
    scores = jnp.einsum("hqc,hkc->hqk", q_blk, k_heads, preferred_element_type=jnp.float32) * scale
    allowed = (seg_rows[:, None] == seg_cols[None, :]) & (col_pos[None, :] <= row_pos[:, None])
    return jnp.where(allowed[None], scores, NEG_BIG)


def attention_forward(q_heads, k_heads, v_heads, seg_ids):
    head_count = q_heads.shape[0]
    row_total = q_heads.shape[1]
    block_rows = min(row_total, BLOCK_ROWS)
    block_count = row_total // block_rows
    col_pos = jnp.arange(row_total, dtype=jnp.int32)

    def one_block(start):
        row_pos = start + jnp.arange(block_rows, dtype=jnp.int32)
        scores = masked_scores(q_heads, k_heads, seg_ids, seg_ids, row_pos, col_pos)
        top_score = jnp.max(scores, axis=-1, keepdims=True)
        log_total = top_score + jnp.log(
            jnp.sum(jnp.exp(scores - top_score), axis=-1, keepdims=True)
        )
        prob_low = jnp.exp(scores - log_total).astype(jnp.bfloat16)
        attended = jnp.einsum("hqk,hkd->hqd", prob_low, v_heads, preferred_element_type=jnp.float32)
        return (attended.astype(jnp.bfloat16), log_total)

    starts = jnp.arange(block_count, dtype=jnp.int32) * block_rows
    attended, log_total = lax.map(one_block, starts)
    attended = attended.transpose(1, 0, 2, 3).reshape(head_count, row_total, -1)
    log_total = log_total.transpose(1, 0, 2, 3).reshape(head_count, row_total, 1)
    return (attended, log_total)


def attention_backward(q_heads, k_heads, v_heads, grad_att, log_total, seg_ids):
    scale = (DH + DR) ** (-0.5)
    head_count = q_heads.shape[0]
    row_total = q_heads.shape[1]
    block_rows = min(row_total, BLOCK_ROWS)
    block_count = row_total // block_rows
    col_pos = jnp.arange(row_total, dtype=jnp.int32)

    def one_block(carry, start):
        grad_k_acc, grad_v_acc = carry
        row_pos = start + jnp.arange(block_rows, dtype=jnp.int32)
        scores = masked_scores(q_heads, k_heads, seg_ids, seg_ids, row_pos, col_pos)
        prob_full = jnp.exp(scores - log_total)
        prob_low = prob_full.astype(jnp.bfloat16)
        grad_v_blk = jnp.einsum(
            "hqk,hqd->hkd", prob_low, grad_att, preferred_element_type=jnp.float32
        )
        grad_prob = jnp.einsum(
            "hqd,hkd->hqk", grad_att, v_heads, preferred_element_type=jnp.float32
        )
        row_dot = jnp.sum(prob_full * grad_prob, axis=-1, keepdims=True)
        grad_scores = (prob_full * (grad_prob - row_dot) * scale).astype(jnp.bfloat16)
        grad_q_blk = jnp.einsum(
            "hqk,hkc->hqc", grad_scores, k_heads, preferred_element_type=jnp.float32
        )
        grad_k_blk = jnp.einsum(
            "hqk,hqc->hkc", grad_scores, q_heads, preferred_element_type=jnp.float32
        )
        return ((grad_k_acc + grad_k_blk, grad_v_acc + grad_v_blk), grad_q_blk)

    starts = jnp.arange(block_count, dtype=jnp.int32) * block_rows
    init_acc = (jnp.zeros(k_heads.shape, jnp.float32), jnp.zeros(v_heads.shape, jnp.float32))
    (grad_k, grad_v), grad_q_blocks = lax.scan(one_block, init_acc, starts)
    grad_q = grad_q_blocks.transpose(1, 0, 2, 3).reshape(head_count, row_total, -1)
    return (grad_q, grad_k, grad_v)


MESH_IDS = pl.DeviceIdType.MESH
LOW = jnp.bfloat16
NT = (((1,), (1,)), ((), ()))
TN = (((0,), (0,)), ((), ()))


def axis_parts(mesh):
    devices = mesh.devices
    found = []
    for axis in range(devices.ndim):
        first = (0,) * devices.ndim
        line = [devices[first[:axis] + (i,) + first[axis + 1 :]] for i in range(devices.shape[axis])]
        places = [(*dev.coords, dev.core_on_chip) for dev in line]
        parts = []
        for k, name in enumerate(("x", "y", "z", "core")):
            values = [p[k] for p in places]
            if len(set(values)) > 1:
                stride = next(i for i, v in enumerate(values) if v != values[0])
                parts.append((stride, name, len(set(values))))
        found.append(tuple((name, size) for stride, name, size in sorted(parts, reverse=True)))
    return tuple(found)


def fits_kernels(mesh):
    wide, narrow = axis_parts(mesh)
    return (
        len(wide) == 2
        and wide[1][1] == 2
        and len(narrow) == 2
        and narrow[0][1] == 2
        and narrow[1] == ("core", 2)
    )


class Spot:
    def __init__(self, line):
        wide, narrow = lax.axis_index("wide"), lax.axis_index("narrow")
        self.line = line
        self.z, self.x = wide // 2, wide % 2
        self.y, self.c = narrow // 2, narrow % 2

    def wide(self, z, xf=0):
        return z * 2 + self.x + xf * (1 - 2 * self.x)

    def narrow(self, yf=0, cf=0):
        return (self.y + yf * (1 - 2 * self.y)) * 2 + self.c + cf * (1 - 2 * self.c)

    def device(self, z, xf=0, yf=0, cf=0):
        return {"wide": self.wide(z, xf), "narrow": self.narrow(yf, cf)}

    def flips(self, a, b, c):
        return a * (1 - c) + b * c, b * (1 - c) + a * c

    def index(self, z, a, b, cf=0):
        xf, yf = self.flips(a, b, self.c + cf * (1 - 2 * self.c))
        return self.wide(z, xf) * 4 + self.narrow(yf, cf)

    def routed(self, z, a, b):
        xf, yf = self.flips(a, b, self.c)
        return self.device(z, xf, yf)

    def inside(self, z):
        return (z >= 0) & (z < self.line)

    def near(self, rank):
        table = [sorted(range(self.line), key=lambda to: (abs(to - at), to))[rank] for at in range(self.line)]
        found = jnp.int32(table[0])
        for at in range(1, self.line):
            found = jnp.where(self.z == at, table[at], found)
        return found


def enter(spot, line_too, flips, wide_count=0):
    barrier = pltpu.get_barrier_semaphore()
    devices = [spot.device(spot.z, *flip) for flip in flips]
    if wide_count:
        here = spot.wide(spot.z)
        devices += [
            {"wide": lax.rem(here + step, wide_count), "narrow": spot.narrow()} for step in range(1, wide_count)
        ]
        devices = [dev for flip, dev in zip(flips, devices) if flip != (1, 0, 0)] + devices[len(flips) :]
        line_too = False
    for dev in devices:
        pl.semaphore_signal(barrier, inc=1, device_id=dev, device_id_type=MESH_IDS)
    if not line_too:
        pl.semaphore_wait(barrier, len(devices))
        return
    for step in (-1, 1):
        @pl.when(spot.inside(spot.z + step))
        def _():
            pl.semaphore_signal(barrier, inc=1, device_id=spot.device(spot.z + step), device_id_type=MESH_IDS)
    inner = spot.inside(spot.z - 1) & spot.inside(spot.z + 1)
    @pl.when(inner)
    def _():
        pl.semaphore_wait(barrier, len(devices) + 2)
    @pl.when(jnp.logical_not(inner))
    def _():
        pl.semaphore_wait(barrier, len(devices) + 1)


class Flow:
    def __init__(self, spot, kind, own, place, send, recv):
        self.spot, self.kind, self.own, self.place, self.send, self.recv = spot, kind, own, place, send, recv
        self.sent = []

    @staticmethod
    def steps(kind, line):
        ranks = (0,) if kind == "narrow" else range(line)
        firsts = (0,) if kind == "narrow" else (0, 1)
        seconds = (0,) if kind in ("wide", "wide2") else (0, 1)
        steps = [(r, a, b) for r in ranks for a in firsts for b in seconds]
        return sorted(steps, key=lambda s: (s[0] + s[1] + 2 * s[2], s[1], s[2]))

    @staticmethod
    def sends(kind, rank, a, b):
        along = kind != "narrow" and (kind in ("all2", "wide2") or not (a or b))
        moves = ["up", "down"] if along else []
        fresh = not rank or kind in ("all", "wide", "narrow")
        if kind != "narrow" and fresh and not a and not b:
            moves.append("a")
        if kind not in ("wide", "wide2") and fresh and not b:
            moves.append("b")
        if kind not in ("wide", "wide2"):
            moves.append("core")
        return moves

    @classmethod
    def send_count(cls, kind, line):
        return sum(len(cls.sends(kind, *step)) for step in cls.steps(kind, line))

    @staticmethod
    def blocks(kind, line):
        return {"all": line * 8, "all2": line * 8, "wide": line * 2, "wide2": line * 2, "narrow": 4}[kind]

    def block(self, z, a, b, cf=0):
        if self.kind in ("all", "all2"):
            return self.spot.index(z, a, b, cf)
        return self.spot.narrow(b, cf) if self.kind == "narrow" else self.spot.wide(z, a)

    def target(self, move):
        spot = self.spot
        if move in ("up", "down"):
            return spot.device(spot.z + (1 if move == "up" else -1))
        if move == "core":
            return spot.device(spot.z, 0, 0, 1)
        if self.kind in ("all", "all2"):
            return spot.routed(spot.z, int(move == "a"), int(move == "b"))
        return spot.device(spot.z, int(move == "a"), int(move == "b"))

    def copy(self, block, move, number, first=False):
        view = self.place(block)
        return pltpu.make_async_remote_copy(
            src_ref=self.own if first else view,
            dst_ref=view,
            send_sem=self.send.at[number],
            recv_sem=self.recv.at[block],
            device_id=self.target(move),
            device_id_type=MESH_IDS,
        )

    def arrive(self, block):
        self.copy(block, "a" if self.kind in ("wide", "wide2") else "core", 0).wait_recv()

    def step(self, rank, a, b):
        spot = self.spot
        z = spot.z if rank == 0 else spot.near(rank)
        block = self.block(z, a, b)
        first = rank == 0 and not a and not b
        if not first:
            self.arrive(block)
        for move in self.sends(self.kind, rank, a, b):
            copy = self.copy(block, move, len(self.sent), first)
            when = None
            if move == "up":
                when = spot.inside(spot.z + 1) & (z <= spot.z)
            elif move == "down":
                when = spot.inside(spot.z - 1) & (z >= spot.z)
            if when is None:
                copy.start()
            else:
                pl.when(when)(copy.start)
            self.sent.append((when, copy))

    def from_core(self, z, a, b):
        self.arrive(self.block(z, a, b, 1))

    def finish(self):
        for when, copy in self.sent:
            if when is None:
                copy.wait_send()
            else:
                pl.when(when)(copy.wait_send)


class NarrowSum:
    def __init__(self, spot, rows, part, refs):
        self.spot, self.rows, self.part = spot, rows, part
        (self.held, self.summed, self.core_buf, self.y_buf, self.load_sem, self.core_send, self.core_recv,
         self.y_send, self.y_recv) = refs

    @staticmethod
    def scratch(rows, width, dtype):
        dma = pltpu.SemaphoreType.DMA
        return [
            *(pltpu.VMEM(shape, dtype) for shape in ((2, rows, width), (rows, width), (2, rows, width), (rows, width))),
            *(dma((2,)) for _ in range(3)),
            dma,
            dma,
        ]

    def block(self, yf, cf):
        start = pl.multiple_of(self.spot.narrow(yf, cf) * self.rows, self.rows)
        return self.part.at[pl.ds(start, self.rows), :]

    def to_core(self, yf):
        return pltpu.make_async_remote_copy(
            src_ref=self.block(yf, 1), dst_ref=self.core_buf.at[yf], send_sem=self.core_send.at[yf],
            recv_sem=self.core_recv.at[yf], device_id=self.spot.device(self.spot.z, 0, 0, 1), device_id_type=MESH_IDS,
        )

    def load(self, yf):
        return pltpu.make_async_copy(self.block(yf, 0), self.held.at[yf], self.load_sem.at[yf])

    def over_y(self):
        return pltpu.make_async_remote_copy(
            src_ref=self.summed, dst_ref=self.y_buf, send_sem=self.y_send, recv_sem=self.y_recv,
            device_id=self.spot.device(self.spot.z, 0, 1, 0), device_id_type=MESH_IDS,
        )

    def start(self):
        for yf in (1, 0):
            self.to_core(yf).start()
            self.load(yf).start()

    def joined(self, yf):
        self.load(yf).wait()
        self.to_core(yf).wait_recv()
        return self.held[yf].astype(jnp.float32) + self.core_buf[yf].astype(jnp.float32)

    def send(self):
        self.summed[...] = self.joined(1).astype(self.summed.dtype)
        self.over_y().start()

    def total(self):
        value = self.joined(0)
        self.over_y().wait_recv()
        return value + self.y_buf[...].astype(jnp.float32)

    def finish(self):
        self.over_y().wait_send()
        for yf in (1, 0):
            self.to_core(yf).wait_send()


def latent_back(value, lat, cos_sin, lat_gain, w_lat, w_rope, tokens, gain, grad_resid):
    width, lat_width = tokens.shape[1], lat.shape[1]
    at = width + lat_width
    grad_x, grad_lat = value[:, :width], value[:, width:at]
    rope = value[:, at : at + 128] * cos_sin[0] + value[:, at + 128 :] * cos_sin[1]
    inv = lax.rsqrt(jnp.mean(lat * lat, axis=-1, keepdims=True) + EPS)
    scaled = grad_lat * lat_gain
    down = inv * scaled - lat * inv**3 * jnp.mean(lat * scaled, axis=-1, keepdims=True)
    lat_terms = jnp.sum(grad_lat * lat * inv, axis=0, keepdims=True)
    lat_low, rope_low = down.astype(LOW), rope.astype(LOW)
    grad_x += jnp.dot(lat_low, w_lat, preferred_element_type=jnp.float32)
    grad_x += jnp.dot(rope_low[:, :DR], w_rope, preferred_element_type=jnp.float32)
    x = tokens.astype(jnp.float32)
    inv = lax.rsqrt(jnp.mean(x * x, axis=-1, keepdims=True) + EPS)
    scaled = grad_x * gain
    back = inv * scaled - x * inv**3 * jnp.mean(x * scaled, axis=-1, keepdims=True)
    gain_terms = jnp.sum(grad_x * x * inv, axis=0, keepdims=True)
    return (back + grad_resid).astype(LOW), lat_low, rope_low, gain_terms, lat_terms


class WideSum:
    def __init__(self, spot, take, src, dst, refs):
        self.spot, self.take, self.src, self.dst = spot, take, src, dst
        (self.stage, self.x_buf, self.z_buf, self.total, self.x_send, self.x_recv, self.z_send, self.z_recv,
         self.out_sem) = refs

    @staticmethod
    def scratch(line, block, dtype):
        dma = pltpu.SemaphoreType.DMA
        return [
            pltpu.VMEM((line, *block), dtype),
            pltpu.VMEM((line, *block), dtype),
            pltpu.VMEM((line * 2, *block), dtype),
            pltpu.VMEM(block, jnp.float32),
            *(dma((n,)) for n in (line, line, line, line * 2)),
            dma,
        ]

    def zed(self, j):
        rank = self.spot.line - 1 - j
        return self.spot.z if rank == 0 else self.spot.near(rank)

    def to_x(self, z):
        return pltpu.make_async_remote_copy(
            src_ref=self.take(self.src, self.spot.wide(z, 1)), dst_ref=self.x_buf.at[z],
            send_sem=self.x_send.at[z], recv_sem=self.x_recv.at[z],
            device_id=self.spot.device(self.spot.z, 1), device_id_type=MESH_IDS,
        )

    def to_z(self, z, down):
        return pltpu.make_async_remote_copy(
            src_ref=self.stage.at[z], dst_ref=self.z_buf.at[down * self.spot.line + z],
            send_sem=self.z_send.at[z], recv_sem=self.z_recv.at[down * self.spot.line + z],
            device_id=self.spot.device(self.spot.z + 1 - 2 * down), device_id_type=MESH_IDS,
        )

    def start(self):
        for j in range(self.spot.line):
            self.to_x(self.zed(j)).start()

    def step(self, j):
        spot = self.spot
        z = self.zed(j)
        last = j == spot.line - 1
        self.to_x(z).wait_recv()
        value = self.take(self.src, spot.wide(z))[...].astype(jnp.float32) + self.x_buf[z].astype(jnp.float32)
        if last:
            self.total[...] = value
        else:
            self.stage[z] = value.astype(self.stage.dtype)
        for down in (0, 1):
            behind = spot.inside(spot.z - 1 + 2 * down)
            if last:
                @pl.when(behind)
                def _():
                    self.to_z(z, down).wait_recv()
                    self.total[...] += self.z_buf[down * spot.line + z].astype(jnp.float32)
            else:
                @pl.when((z < spot.z) if down else (z > spot.z))
                def _():
                    @pl.when(behind)
                    def _():
                        self.to_z(z, down).wait_recv()
                        more = self.stage[z].astype(jnp.float32) + self.z_buf[down * spot.line + z].astype(jnp.float32)
                        self.stage[z] = more.astype(self.stage.dtype)
                    self.to_z(z, down).start()
        if last:
            pltpu.make_async_copy(self.total, self.dst, self.out_sem).start()

    def finish(self):
        spot = self.spot
        for j in range(spot.line):
            z = self.zed(j)
            self.to_x(z).wait_send()
            if j < spot.line - 1:
                for down in (0, 1):
                    @pl.when((z < spot.z) if down else (z > spot.z))
                    def _():
                        self.to_z(z, down).wait_send()
        pltpu.make_async_copy(self.total, self.dst, self.out_sem).wait()


def cut_of(ref, axis, start, size):
    return ref.at[tuple(pl.ds(start, size) if k == axis else slice(None) for k in range(len(ref.shape)))]


def routes(item):
    kind, split = item["kind"], item["split"]
    if split is None:
        return [(kind, None)]
    axis, first = split
    return [(kind, (axis, 0, first)), (kind + "2", (axis, first, item["array"].shape[axis] - first))]


def swap_sends(item, line):
    return {"wswap": line * 2, "nswap": 4}[item["kind"]]


def item_scratch(item, line):
    dma = pltpu.SemaphoreType.DMA
    if item["kind"] == "wsum":
        return WideSum.scratch(line, item["shape"], item["array"].dtype)
    if item["kind"] in ("wswap", "nswap"):
        return [dma((swap_sends(item, line),)), dma((swap_sends(item, line),))]
    return [
        sem
        for kind, _ in routes(item)
        for sem in (dma((Flow.send_count(kind, line),)), dma((Flow.blocks(kind, line),)))
    ]


def move_kernel(line, items, front_count, *refs):
    count = len(items)
    given = [i for i, item in enumerate(items) if not item.get("late")]
    srcs = dict(zip(given, refs))
    front, refs = refs[len(given) : len(given) + front_count], refs[len(given) + front_count :]
    dsts, local, rest = refs[:count], refs[count], list(refs[count + 1 :])
    late = [i for i in range(count) if i not in given]
    for i in late:
        srcs[i] = rest.pop(0)
    spot = Spot(line)
    if front_count:
        terms, lat, cos_sin, lat_gain, w_lat, w_rope, tokens, gain, grad_resid, ffn_terms = front
        narrow = NarrowSum(spot, terms.shape[0] // 4, terms, [rest.pop(0) for _ in range(9)])
    kinds = [item["kind"] for item in items]
    flips = set()
    for kind in kinds:
        flips |= {
            "all": {(1, 0, 0), (0, 1, 0), (0, 0, 1)},
            "wide": {(1, 0, 0)},
            "narrow": {(0, 1, 0), (0, 0, 1)},
            "wswap": set(),
            "nswap": {(0, 1, 0), (0, 0, 1), (0, 1, 1)},
            "wsum": {(1, 0, 0)},
        }[kind]
    wide_count = line * 2
    swaps = any(kind == "wswap" for kind in kinds)
    enter(spot, any(k in ("all", "wide", "wsum") for k in kinds), sorted(flips), wide_count if swaps else 0)
    here_wide, here_narrow = spot.wide(spot.z), spot.narrow()

    flows, sums, copies, own, own_late, held_back = [], [], [], [], [], []
    if front_count:
        narrow.start()
    for i, item in enumerate(items):
        refs_of = [rest.pop(0) for _ in item_scratch(item, line)]
        put, take = item["put"], item["take"]
        if item["kind"] == "wsum":
            sums.append(WideSum(spot, take, srcs[i], dsts[i], refs_of))
            continue
        if item["kind"] not in ("wswap", "nswap"):
            for n, (kind, cut) in enumerate(routes(item)):

                def place(block, i=i, put=put, cut=cut):
                    view = put(dsts[i], block)
                    return view if cut is None else cut_of(view, *cut)

                part = srcs[i] if cut is None else cut_of(srcs[i], *cut)
                flows.append(Flow(spot, kind, part, place, *refs_of[2 * n : 2 * n + 2]))
                if i in late:
                    held_back.append(flows[-1])
            (own_late if i in late else own).append(
                pltpu.make_async_copy(srcs[i], put(dsts[i], flows[-1].block(spot.z, 0, 0)), local.at[i])
            )
            continue
        send, recv = refs_of
        if item["kind"] == "wswap":
            here = here_wide
            peers = [lax.rem(here + k, wide_count) for k in range(1, wide_count)]
            devices = [{"wide": to, "narrow": here_narrow} for to in peers]
        else:
            here = here_narrow
            ways = ((0, 1), (1, 0), (1, 1))
            peers = [spot.narrow(*way) for way in ways]
            devices = [spot.device(spot.z, 0, *way) for way in ways]
        for k, (to, dev) in enumerate(zip(peers, devices)):
            src = take(srcs[i], to)
            copies.append(tuple(
                pltpu.make_async_remote_copy(
                    src_ref=src, dst_ref=put(dsts[i], at), send_sem=send.at[k], recv_sem=recv.at[at],
                    device_id=dev, device_id_type=MESH_IDS,
                )
                for at in (here, to)
            ))
        own.append(pltpu.make_async_copy(take(srcs[i], here), put(dsts[i], here), local.at[i]))
    steps = sorted(
        ((step, flow) for flow in flows for step in Flow.steps(flow.kind, line)),
        key=lambda s: s[0][0] + s[0][1] + 2 * s[0][2],
    )
    for step, flow in steps:
        if step == (0, 0, 0) and flow not in held_back:
            flow.step(*step)
    for one in sums:
        one.start()
    for copy in own:
        copy.start()
    if front_count:
        narrow.send()
        values = latent_back(
            narrow.total(), lat[...], cos_sin[...], lat_gain[...], w_lat[...], w_rope[...], tokens[...], gain[...],
            grad_resid[...],
        )
        rows_to, lat_to, rope_to, gains_to = (srcs[i] for i in late)
        rows_to[...], lat_to[...], rope_to[...] = values[:3]
        width = gain.shape[1]
        gains_to[:, :width] = values[3]
        gains_to[:, width : 2 * width] = ffn_terms[...]
        gains_to[:, 2 * width :] = values[4]
        for flow in held_back:
            flow.step(0, 0, 0)
        for copy in own_late:
            copy.start()
    level = 0
    for step, flow in steps:
        if sum(step) > level:
            if level == 1:
                for out, _ in copies:
                    out.start()
            if level and level <= line:
                for one in sums:
                    one.step(level - 1)
            level += 1
        if step != (0, 0, 0):
            flow.step(*step)
    for late in range(max(level, 1), line + 1):
        for one in sums:
            one.step(late - 1)
    for flow in flows:
        if flow.kind not in ("wide", "wide2"):
            for rank, a, b in Flow.steps(flow.kind, line):
                flow.from_core(spot.z if rank == 0 else spot.near(rank), a, b)
    for _, back in copies:
        back.wait_recv()
    for flow in (*flows, *sums, *([narrow] if front_count else [])):
        flow.finish()
    for out, _ in copies:
        out.wait_send()
    for copy in (*own, *own_late):
        copy.wait()


def move(line, items, collective_id, front=()):
    moved = sum(item["array"].size * item["array"].dtype.itemsize for item in items) * line * 2
    given = [i for i, item in enumerate(items) if not item.get("late")]
    hbm, vmem = pl.BlockSpec(memory_space=pl.ANY), pl.BlockSpec(memory_space=pltpu.VMEM)
    return pl.pallas_call(
        functools.partial(move_kernel, line, items, len(front)),
        out_shape=[
            jax.ShapeDtypeStruct(item["shape"], jnp.float32 if item["kind"] == "wsum" else item["array"].dtype)
            for item in items
        ],
        in_specs=[vmem] * len(given) + ([hbm] + [vmem] * (len(front) - 1) if front else []),
        out_specs=[hbm] * len(items),
        scratch_shapes=[pltpu.SemaphoreType.DMA((len(items),))]
        + [pltpu.VMEM(item["array"].shape, item["array"].dtype) for item in items if item.get("late")]
        + (NarrowSum.scratch(front[0].shape[0] // 4, front[0].shape[1], front[0].dtype) if front else [])
        + [ref for item in items for ref in item_scratch(item, line)],
        compiler_params=pltpu.CompilerParams(collective_id=collective_id, has_side_effects=True),
        cost_estimate=pl.CostEstimate(flops=0, bytes_accessed=moved, transcendentals=0),
        name="move_blocks",
    )(*[items[i]["array"] for i in given], *front)


def narrow_sum_kernel(line, rows, part, out, held, summed, from_core, from_y,
                      load_sem, core_send, core_recv, y_send, y_recv):
    spot = Spot(line)
    enter(spot, False, [(0, 0, 1), (0, 1, 0)])

    def block(yf, cf):
        return part.at[pl.ds(pl.multiple_of(spot.narrow(yf, cf) * rows, rows), rows), :]

    def to_core(yf):
        return pltpu.make_async_remote_copy(
            src_ref=block(yf, 1), dst_ref=from_core.at[yf], send_sem=core_send.at[yf], recv_sem=core_recv.at[yf],
            device_id=spot.device(spot.z, 0, 0, 1), device_id_type=MESH_IDS,
        )

    def load(yf):
        return pltpu.make_async_copy(block(yf, 0), held.at[yf], load_sem.at[yf])

    over_y = pltpu.make_async_remote_copy(
        src_ref=summed, dst_ref=from_y, send_sem=y_send, recv_sem=y_recv,
        device_id=spot.device(spot.z, 0, 1, 0), device_id_type=MESH_IDS,
    )
    for yf in (1, 0):
        to_core(yf).start()
        load(yf).start()
    load(1).wait()
    to_core(1).wait_recv()
    summed[...] = (held[1].astype(jnp.float32) + from_core[1].astype(jnp.float32)).astype(summed.dtype)
    over_y.start()
    load(0).wait()
    to_core(0).wait_recv()
    total = held[0].astype(jnp.float32) + from_core[0].astype(jnp.float32)
    over_y.wait_recv()
    out[...] = total + from_y[...].astype(jnp.float32)
    over_y.wait_send()
    for yf in (1, 0):
        to_core(yf).wait_send()


def narrow_sum(line, part, collective_id):
    rows, width = part.shape[0] // 4, part.shape[1]
    dma = pltpu.SemaphoreType.DMA
    return pl.pallas_call(
        functools.partial(narrow_sum_kernel, line, rows),
        out_shape=jax.ShapeDtypeStruct((rows, width), jnp.float32),
        in_specs=[pl.BlockSpec(memory_space=pl.ANY)],
        out_specs=pl.BlockSpec(memory_space=pltpu.VMEM),
        scratch_shapes=[
            pltpu.VMEM((2, rows, width), part.dtype),
            pltpu.VMEM((rows, width), part.dtype),
            pltpu.VMEM((2, rows, width), part.dtype),
            pltpu.VMEM((rows, width), part.dtype),
            dma((2,)),
            dma((2,)),
            dma((2,)),
            dma,
            dma,
        ],
        compiler_params=pltpu.CompilerParams(collective_id=collective_id, has_side_effects=True),
        cost_estimate=pl.CostEstimate(
            flops=part.size, bytes_accessed=2 * part.size * part.dtype.itemsize, transcendentals=0
        ),
        name="narrow_sum",
    )(part)


def rows_in_kernel(line, sizes, hid_own, grad_own, gates, w_up, s_up, w_down, s_down,
                   hid_all, grad_all, act_e, act_s, dgu_e, dgu_s,
                   land_h, land_g, v_up, v_sup, v_down, v_sdown, t_act, t_sact, t_dgu, t_sdgu,
                   in_sem, own_sem, keep_sem, out_sem, *sems):
    rows, experts, hid, shared, first = sizes
    h_sems, g_sems = sems[:4], sems[4:]
    group = 4 * rows
    spot = Spot(line)
    loads = [
        pltpu.make_async_copy(src, dst, in_sem.at[i])
        for i, (src, dst) in enumerate(((w_up, v_up), (w_down, v_down), (s_up, v_sup), (s_down, v_sdown)))
    ]
    for copy in loads:
        copy.start()
    enter(spot, True, [(0, 0, 1), (0, 1, 0), (1, 0, 0)])

    def place(land, cut, block):
        return land.at[pl.ds(pl.multiple_of(block * rows, rows), rows), cut]

    width = hid_own.shape[1]
    cuts = (("all", pl.ds(0, first)), ("all2", pl.ds(first, width - first)))
    flows = [
        Flow(spot, kind, src.at[:, cut], functools.partial(place, land, cut), send, recv)
        for src, land, sems in ((hid_own, land_h, h_sems), (grad_own, land_g, g_sems))
        for (kind, cut), (send, recv) in zip(cuts, (sems[:2], sems[2:]))
    ]
    for flow in flows:
        flow.step(0, 0, 0)
    mine = flows[0].block(spot.z, 0, 0)
    own = [
        pltpu.make_async_copy(hid_own, place(land_h, slice(None), mine), own_sem.at[0]),
        pltpu.make_async_copy(grad_own, place(land_g, slice(None), mine), own_sem.at[1]),
    ]
    for copy in own:
        copy.start()

    def keeps(n, at):
        span = pl.ds(pl.multiple_of(at * group, group), group)
        return (
            pltpu.make_async_copy(land_h.at[span, :], hid_all.at[span, :], keep_sem.at[0, n]),
            pltpu.make_async_copy(land_g.at[span, :], grad_all.at[span, :], keep_sem.at[1, n]),
        )

    def stores(n, at):
        cols = pl.ds(pl.multiple_of(at * group, group), group)
        slot = n % 2
        pairs = (
            (t_act.at[slot], act_e.at[:, cols], out_sem.at[0, slot]),
            (t_sact.at[slot], act_s.at[:, cols], out_sem.at[1, slot]),
            (t_dgu.at[slot], dgu_e.at[:, cols], out_sem.at[2, slot]),
            (t_sdgu.at[slot], dgu_s.at[:, cols], out_sem.at[3, slot]),
        )
        return [pltpu.make_async_copy(*pair) for pair in pairs]

    def both_ways(gate_part, up_part, grad_part, gate):
        sig = 1.0 / (1.0 + jnp.exp(-gate_part))
        silu = gate_part * sig
        if gate is not None:
            grad_part = grad_part * gate
        grad_gate = grad_part * up_part * (sig + silu * (1.0 - sig))
        act = silu * up_part
        if gate is not None:
            act = act * gate
        return act.astype(LOW), grad_gate.astype(LOW), (grad_part * silu).astype(LOW)

    done = []

    def compute(at):
        n = len(done)
        if n >= 2:
            for copy in stores(n - 2, done[n - 2]):
                copy.wait()
        slot = n % 2
        cols = pl.ds(pl.multiple_of(at * group, group), group)
        h, g = land_h[cols, :], land_g[cols, :]
        for e in range(experts):
            gu = lax.dot_general(
                v_up[2 * e * hid : 2 * (e + 1) * hid, :], h, NT, preferred_element_type=jnp.float32
            )
            da = lax.dot_general(v_down[e * hid : (e + 1) * hid, :], g, NT, preferred_element_type=jnp.float32)
            act, dg, du = both_ways(gu[:hid], gu[hid:], da, gates[e : e + 1, cols])
            t_act[slot, e * hid : (e + 1) * hid, :] = act
            t_dgu[slot, 2 * e * hid : (2 * e + 1) * hid, :] = dg
            t_dgu[slot, (2 * e + 1) * hid : 2 * (e + 1) * hid, :] = du
        gu = lax.dot_general(v_sup[...], h, NT, preferred_element_type=jnp.float32)
        da = lax.dot_general(v_sdown[...], g, NT, preferred_element_type=jnp.float32)
        act, dg, du = both_ways(gu[:shared], gu[shared:], da, None)
        t_sact[slot] = act
        t_sdgu[slot, :shared, :] = dg
        t_sdgu[slot, shared:, :] = du
        done.append(at)
        for copy in (*keeps(n, at), *stores(n, at)):
            copy.start()

    waiting = sorted(
        ((s[0] + s[1] + 2 * s[2], s) for s in Flow.steps("all", line) if s != (0, 0, 0)), key=lambda s: s[0]
    )
    loaded = False
    for _, (rank, a, b) in waiting:
        for flow in flows:
            flow.step(rank, a, b)
        if a and b:
            z = spot.z if rank == 0 else spot.near(rank)
            if not loaded:
                loaded = True
                for copy in own + loads:
                    copy.wait()
            for xf in (0, 1):
                for flow in flows:
                    for other in (0, 1):
                        ca = xf * spot.c + other * (1 - spot.c)
                        cb = other * spot.c + xf * (1 - spot.c)
                        flow.from_core(z, ca, cb)
                compute(spot.wide(z, xf))
    for flow in flows:
        flow.finish()
    count = len(done)
    for n, at in enumerate(done):
        for copy in (*keeps(n, at), *(stores(n, at) if n >= count - 2 else ())):
            copy.wait()


def rows_in(line, hid_own, grad_own, gates, w_up, s_up, w_down, s_down, experts, collective_id):
    rows, width = hid_own.shape
    tokens = rows * line * 8
    hid, shared = w_down.shape[0] // experts, s_down.shape[0]
    group = 4 * rows
    dma = pltpu.SemaphoreType.DMA
    hbm = pl.BlockSpec(memory_space=pl.ANY)
    vmem = pl.BlockSpec(memory_space=pltpu.VMEM)
    first = width * 13 // 16 // 128 * 128
    flow_sems = [dma((n,)) for kind in ("all", "all2") for n in (Flow.send_count(kind, line), line * 8)]
    out = [(tokens, width), (tokens, width)]
    out += [(f, tokens) for f in (w_down.shape[0], shared, w_up.shape[0], 2 * shared)]
    return pl.pallas_call(
        functools.partial(rows_in_kernel, line, (rows, experts, hid, shared, first)),
        out_shape=[jax.ShapeDtypeStruct(shape, LOW) for shape in out],
        in_specs=[vmem, vmem, vmem] + [hbm] * 4,
        out_specs=[hbm] * 6,
        scratch_shapes=[pltpu.VMEM((tokens, width), LOW)] * 2
        + [pltpu.VMEM(arr.shape, LOW) for arr in (w_up, s_up, w_down, s_down)]
        + [pltpu.VMEM((2, f, group), LOW) for f in (w_down.shape[0], shared, w_up.shape[0], 2 * shared)]
        + [
            dma((4,)),
            dma((2,)),
            dma((2, line * 2)),
            dma((4, 2)),
            *flow_sems,
            *flow_sems,
        ],
        compiler_params=pltpu.CompilerParams(
            collective_id=collective_id, has_side_effects=True, vmem_limit_bytes=60 << 20
        ),
        cost_estimate=pl.CostEstimate(
            flops=6 * (w_down.shape[0] + shared) * tokens * width,
            bytes_accessed=6 * tokens * width,
            transcendentals=(w_down.shape[0] + shared) * tokens,
        ),
        name="rows_in",
    )(hid_own, grad_own, gates, w_up, s_up, w_down, s_down)


class Sum:
    def __init__(self, spot, rows, lhs, w, loads, refs):
        self.spot, self.rows, self.lhs, self.w, self.loads = spot, rows, lhs, w, loads
        (self.stage, self.core_buf, self.b_buf, self.a_buf, self.z_buf,
         self.core_send, self.core_recv, self.b_send, self.b_recv, self.a_send, self.a_recv,
         self.z_send, self.z_recv) = refs

    def zed(self, j):
        rank = self.spot.line - 1 - j
        return self.spot.z if rank == 0 else self.spot.near(rank)

    def group(self, xf, j):
        z = self.zed(j)
        return z, self.spot.wide(z, xf)

    def place(self, at, yf, cf):
        start = pl.multiple_of(self.spot.narrow(yf, cf) * self.rows, self.rows)
        return self.stage.at[at, pl.ds(start, self.rows), :]

    def copy(self, src, dst, send, recv, number, to, device):
        return pltpu.make_async_remote_copy(
            src_ref=src, dst_ref=dst.at[to], send_sem=send.at[number], recv_sem=recv.at[to],
            device_id=device, device_id_type=MESH_IDS,
        )

    def to_core(self, z, at, xf, yf):
        s = (z * 2 + xf) * 2 + yf
        return self.copy(self.place(at, yf, 1), self.core_buf, self.core_send, self.core_recv, s, s,
                         self.spot.device(self.spot.z, 0, 0, 1))

    def to_b(self, z, at, yf, a):
        s = z * 2 + a
        return self.copy(self.place(at, yf, 0), self.b_buf, self.b_send, self.b_recv, s, s,
                         self.spot.routed(self.spot.z, 0, 1))

    def to_a(self, z, at, yf):
        return self.copy(self.place(at, yf, 0), self.a_buf, self.a_send, self.a_recv, z, z,
                         self.spot.routed(self.spot.z, 1, 0))

    def to_z(self, z, at, down):
        return self.copy(self.place(at, 0, 0), self.z_buf, self.z_send, self.z_recv, z, down * self.spot.line + z,
                         self.spot.device(self.spot.z + 1 - 2 * down))

    def only(self, core, act):
        pl.when(self.spot.c == core)(act)

    def produce(self, xf, j, chunk):
        z, at = self.group(xf, j)
        size = 4 * self.rows
        cols = pl.ds(pl.multiple_of(at * size, size), size)
        for copy in self.loads(xf, j, at):
            copy.wait()
        width = self.stage.shape[2]

        @pl.loop(0, width // chunk)
        def _(t):
            cut = pl.ds(pl.multiple_of(t * chunk, chunk), chunk)
            value = sum(
                lax.dot_general(lhs[:, cols], w[:, cut], TN, preferred_element_type=jnp.float32)
                for lhs, w in zip(self.lhs, self.w)
            )
            self.stage[at, :, cut] = value.astype(LOW)

        for yf in (1, 0):
            self.to_core(z, at, xf, yf).start()

    def joined(self, z, at, xf, yf):
        self.to_core(z, at, xf, yf).wait_recv()
        there = self.core_buf[(z * 2 + xf) * 2 + yf]
        return self.place(at, yf, 0)[...].astype(jnp.float32) + there.astype(jnp.float32)

    def send_b(self, xf, yf, a, j):
        z, at = self.group(xf, j)
        self.place(at, yf, 0)[...] = self.joined(z, at, xf, yf).astype(LOW)
        self.to_b(z, at, yf, a).start()

    def send_a(self, xf, yf, j):
        z, at = self.group(xf, j)
        value = self.joined(z, at, xf, yf)
        self.to_b(z, at, yf, 1).wait_recv()
        self.place(at, yf, 0)[...] = (value + self.b_buf[z * 2 + 1].astype(jnp.float32)).astype(LOW)
        self.to_a(z, at, yf).start()

    def send_z(self, j, out):
        spot = self.spot
        z, at = self.group(0, j)
        value = self.joined(z, at, 0, 0)
        self.to_b(z, at, 0, 0).wait_recv()
        self.to_a(z, at, 0).wait_recv()
        value += self.b_buf[z * 2].astype(jnp.float32) + self.a_buf[z].astype(jnp.float32)
        last = j == spot.line - 1
        if last:
            out[...] = value
        else:
            self.place(at, 0, 0)[...] = value.astype(LOW)
        for down in (0, 1):
            behind = spot.inside(spot.z - 1 + 2 * down)
            if last:
                @pl.when(behind)
                def _():
                    self.to_z(z, at, down).wait_recv()
                    out[...] += self.z_buf[down * spot.line + z].astype(jnp.float32)
            else:
                @pl.when((z < spot.z) if down else (z > spot.z))
                def _():
                    @pl.when(behind)
                    def _():
                        self.to_z(z, at, down).wait_recv()
                        more = self.place(at, 0, 0)[...].astype(jnp.float32)
                        more += self.z_buf[down * spot.line + z].astype(jnp.float32)
                        self.place(at, 0, 0)[...] = more.astype(LOW)
                    self.to_z(z, at, down).start()

    def early(self, j):
        self.send_b(1, 1, 1, j)
        self.only(1, lambda: self.send_b(1, 0, 0, j))

    def middle(self, j):
        self.only(0, lambda: self.send_b(0, 1, 0, j))
        self.only(0, lambda: self.send_a(1, 0, j))

    def late(self, j):
        self.only(1, lambda: self.send_a(0, 1, j))

    def finish(self):
        for j in range(self.spot.line):
            for xf in (1, 0):
                z, at = self.group(xf, j)
                for yf in (1, 0):
                    self.to_core(z, at, xf, yf).wait_send()
            z, at = self.group(1, j)
            self.to_b(z, at, 1, 1).wait_send()
            self.only(1, lambda: self.to_b(z, at, 0, 0).wait_send())
            self.only(0, lambda: self.to_a(z, at, 0).wait_send())
            z2, at2 = self.group(0, j)
            self.only(0, lambda: self.to_b(z2, at2, 1, 0).wait_send())
            self.only(1, lambda: self.to_a(z2, at2, 1).wait_send())
            if j < self.spot.line - 1:
                for down in (0, 1):
                    @pl.when((z2 < self.spot.z) if down else (z2 > self.spot.z))
                    def _():
                        self.to_z(z2, at2, down).wait_send()


def rows_out_kernel(line, rows, chunk, count, *refs):
    spot = Spot(line)
    lefts, rights = refs[: 2 * count], refs[2 * count : 4 * count]
    resid, gain, grad_rows = refs[4 * count : 4 * count + 3]
    refs = refs[4 * count + 3 :]
    out, grad_resid, grad_gain, grad_all = refs[:4]
    total, low_rows = refs[4:6]
    refs = refs[6:]
    v_lefts, v_rights = refs[: 2 * count], refs[2 * count : 4 * count]
    rest = refs[4 * count :]
    in_sem, lhs_sem, send, recv, own_sem = rest[:5]
    rest = rest[3:]
    flow = Flow(
        spot, "narrow", low_rows, lambda block: grad_all.at[pl.ds(pl.multiple_of(block * rows, rows), rows), :], send, recv
    )
    own = pltpu.make_async_copy(low_rows, flow.place(spot.narrow()), own_sem)

    def norm_back():
        h, grad = resid[...], total[...]
        inv = lax.rsqrt(jnp.mean(h * h, axis=-1, keepdims=True) + EPS)
        scaled = grad * gain[...]
        value = grad_rows[...].astype(jnp.float32) + inv * scaled
        value -= h * inv**3 * jnp.mean(h * scaled, axis=-1, keepdims=True)
        grad_resid[...] = value
        low_rows[...] = value.astype(LOW)
        grad_gain[...] = jnp.sum(grad * h * inv, axis=0, keepdims=True)
        flow.step(0, 0, 0)
        own.start()

    per = 13
    size = 4 * rows
    right_loads = [pltpu.make_async_copy(rights[k], v_rights[k], in_sem.at[k]) for k in range(2 * count)]

    def loader(s):
        def loads(xf, j, at):
            cols = pl.ds(pl.multiple_of(at * size, size), size)
            return [
                pltpu.make_async_copy(
                    lefts[k].at[:, cols], v_lefts[k].at[:, cols], lhs_sem.at[k, (1 - xf) * line + j]
                )
                for k in (2 * s, 2 * s + 1)
            ]

        return loads

    sums = [
        Sum(spot, rows, v_lefts[2 * s : 2 * s + 2], v_rights[2 * s : 2 * s + 2], loader(s),
            rest[2 + s * per : 2 + (s + 1) * per])
        for s in range(count)
    ]
    for s, one in enumerate(sums):
        for k in (2 * s, 2 * s + 1):
            right_loads[k].start()
        for xf in (1, 0):
            for j in range(line):
                _, at = one.group(xf, j)
                for copy in one.loads(xf, j, at):
                    copy.start()
    enter(spot, True, [(0, 0, 1), (0, 1, 0), (1, 0, 0)])
    ready = set()

    def produce(s, xf, j):
        if s not in ready:
            ready.add(s)
            for k in (2 * s, 2 * s + 1):
                right_loads[k].wait()
        sums[s].produce(xf, j, chunk)

    first, later = sums
    for j in range(line):
        produce(0, 1, j)
        if j:
            first.early(j - 1)
    for j in range(line):
        produce(0, 0, j)
        if j == 0:
            first.early(line - 1)
        else:
            first.middle(j - 1)
    for j in range(line):
        produce(1, 1, j)
        if j == 0:
            first.middle(line - 1)
        else:
            later.early(j - 1)
            first.late(j - 1)
    for j in range(line):
        produce(1, 0, j)
        if j == 0:
            later.early(line - 1)
            first.late(line - 1)
        else:
            later.middle(j - 1)
    later.middle(line - 1)
    for j in range(line - 1):
        first.send_z(j, total)
        later.late(j)
    first.send_z(line - 1, total)
    norm_back()
    later.late(line - 1)
    flow.step(0, 0, 1)
    for j in range(line):
        later.send_z(j, out)
    for b in (0, 1):
        flow.from_core(spot.z, 0, b)
    for one in (*sums, flow):
        one.finish()
    own.wait()


def rows_out(line, pairs, resid, gain, grad_rows, collective_id, chunk=512):
    count = len(pairs)
    lefts = [left for pair in pairs for left, _ in pair]
    rights = [right for pair in pairs for _, right in pair]
    tokens, width = lefts[0].shape[1], rights[0].shape[1]
    rows = tokens // (line * 8)
    dma = pltpu.SemaphoreType.DMA
    slots = line * 4
    scratch = [pltpu.VMEM((rows, width), jnp.float32), pltpu.VMEM((rows, width), LOW)]
    scratch += [pltpu.VMEM(arr.shape, LOW) for arr in lefts + rights] + [dma((2 * count,)), dma((2 * count, line * 2))]
    scratch += [dma((Flow.send_count("narrow", line),)), dma((4,)), dma]
    for _ in range(count):
        scratch += [
            pltpu.VMEM((line * 2, 4 * rows, width), LOW),
            pltpu.VMEM((slots, rows, width), LOW),
            pltpu.VMEM((line * 2, rows, width), LOW),
            pltpu.VMEM((line, rows, width), LOW),
            pltpu.VMEM((line * 2, rows, width), LOW),
            dma((slots,)),
            dma((slots,)),
            dma((line * 2,)),
            dma((line * 2,)),
            dma((line,)),
            dma((line,)),
            dma((line,)),
            dma((line * 2,)),
        ]
    return pl.pallas_call(
        functools.partial(rows_out_kernel, line, rows, chunk, count),
        out_shape=[
            jax.ShapeDtypeStruct((rows, width), jnp.float32),
            jax.ShapeDtypeStruct((rows, width), jnp.float32),
            jax.ShapeDtypeStruct((1, width), jnp.float32),
            jax.ShapeDtypeStruct((4 * rows, width), LOW),
        ],
        in_specs=[pl.BlockSpec(memory_space=pl.ANY)] * (4 * count) + [pl.BlockSpec(memory_space=pltpu.VMEM)] * 3,
        out_specs=[pl.BlockSpec(memory_space=pltpu.VMEM)] * 3 + [pl.BlockSpec(memory_space=pl.ANY)],
        scratch_shapes=scratch,
        compiler_params=pltpu.CompilerParams(
            collective_id=collective_id, has_side_effects=True, vmem_limit_bytes=63 << 20
        ),
        cost_estimate=pl.CostEstimate(
            flops=2 * sum(arr.shape[0] for arr in lefts) * tokens * width,
            bytes_accessed=4 * count * tokens * width,
            transcendentals=0,
        ),
        name="rows_out",
    )(*lefts, *rights, resid, gain, grad_rows)

class Links:
    AXES = {"all": ("wide", "narrow"), "wide": "wide", "narrow": "narrow", "wswap": "wide", "nswap": "narrow"}

    def __init__(self, mesh):
        self.line = axis_parts(mesh)[0][0][1] if fits_kernels(mesh) else None
        self.shape = dict(mesh.shape)
        self.calls = 0

    def number(self):
        self.calls += 1
        return self.calls

    def item(self, array, kind, shape, put, take, plain, split=None):
        return {
            "array": array, "kind": kind, "shape": shape, "put": put, "take": take, "plain": plain, "split": split
        }

    @staticmethod
    def part(axis, size):
        def view(ref, index):
            cut = pl.ds(pl.multiple_of(index * size, size), size)
            return ref.at[tuple(cut if k == axis else slice(None) for k in range(len(ref.shape)))]

        return view

    def count(self, kind):
        return self.shape["wide"] * self.shape["narrow"] if kind == "all" else self.shape[self.AXES[kind]]

    def gather(self, array, kind, axis, split=None):
        shape = list(array.shape)
        shape[axis] *= self.count(kind)
        plain = functools.partial(lax.all_gather, array, self.AXES[kind], axis=axis, tiled=True)
        return self.item(array, kind, tuple(shape), self.part(axis, array.shape[axis]), None, plain, split)

    def wide_sum(self, array, axis):
        shape = list(array.shape)
        shape[axis] //= self.shape["wide"]

        def plain():
            return lax.psum_scatter(array, "wide", scatter_dimension=axis, tiled=True).astype(jnp.float32)

        return self.item(array, "wsum", tuple(shape), None, self.part(axis, shape[axis]), plain)

    def swap(self, array, kind, split, concat):
        count = self.count(kind)
        shape = list(array.shape)
        shape[split] //= count
        size = shape[split]
        put = self.part(concat, array.shape[concat])
        shape[concat] *= count
        plain = functools.partial(
            lax.all_to_all, array, self.AXES[kind], split_axis=split, concat_axis=concat, tiled=True
        )
        return self.item(array, kind, tuple(shape), put, self.part(split, size), plain)

    def grid(self, array):
        rows, cols = array.shape
        down, across = self.shape["narrow"], self.shape["wide"]

        def put(ref, index):
            at_row = pl.multiple_of((index % down) * rows, rows)
            at_col = pl.multiple_of((index // down) * cols, cols)
            return ref.at[pl.ds(at_row, rows), pl.ds(at_col, cols)]

        def plain():
            return lax.all_gather(lax.all_gather(array, "narrow", axis=0, tiled=True), "wide", axis=1, tiled=True)

        return self.item(array, "all", (rows * down, cols * across), put, None, plain)

    def weave(self, array):
        shape = (array.shape[0], self.shape["narrow"], *array.shape[1:])
        plain = functools.partial(lax.all_gather, array, "narrow", axis=1)
        return self.item(array, "narrow", shape, lambda ref, index: ref.at[:, index], None, plain)

    def move_back(self, items, front):
        rows, width = front[8].shape
        lat_width = front[1].shape[1]
        low, full = functools.partial(jax.ShapeDtypeStruct, dtype=LOW), jax.ShapeDtypeStruct
        total = self.count("all")
        if self.line:
            late = [
                self.gather(low((rows, width)), "narrow", 0),
                self.gather(low((rows, lat_width)), "all", 0),
                self.gather(low((rows, 128)), "all", 0),
                self.item(
                    full((1, 2 * width + lat_width), jnp.float32), "all", (total, 1, 2 * width + lat_width),
                    lambda ref, index: ref.at[index], None, None,
                ),
            ]
            late = [{**item, "late": True} for item in late]
            return move(self.line, (*items, *late), self.number(), front)
        summed = lax.psum_scatter(front[0], "narrow", scatter_dimension=0, tiled=True).astype(jnp.float32)
        tokens, lat, rope, gain_terms, lat_terms = latent_back(summed, *front[1:9])
        gains = jnp.concatenate([gain_terms, front[9], lat_terms], 1)
        late = [
            lax.all_gather(tokens, "narrow", axis=0, tiled=True),
            *(lax.all_gather(part, self.AXES["all"], axis=0, tiled=True) for part in (lat, rope)),
            lax.all_gather(gains, self.AXES["all"], axis=0),
        ]
        return [item["plain"]() for item in items] + late

    def move(self, *items):
        if self.line:
            return move(self.line, items, self.number())
        return [item["plain"]() for item in items]

    def narrow_sum(self, part):
        if self.line:
            return narrow_sum(self.line, part, self.number())
        return lax.psum_scatter(part, "narrow", scatter_dimension=0, tiled=True).astype(jnp.float32)

    def rows_in(self, hidden, grad, gates, w_up, s_up, w_down, s_down, experts):
        if self.line:
            return rows_in(self.line, hidden, grad, gates, w_up, s_up, w_down, s_down, experts, self.number())
        hidden, grad = (lax.all_gather(rows, self.AXES["all"], axis=0, tiled=True) for rows in (hidden, grad))

        def both_ways(up, down, gate):
            gu, grad_act = dot_nt(up, hidden), dot_nt(down, grad) * gate
            gate_part, up_part = jnp.split(gu, 2)
            sig = jax.nn.sigmoid(gate_part)
            grad_gate = grad_act * up_part * sig * (1.0 + gate_part * (1.0 - sig))
            grad_up = grad_act * gate_part * sig
            act = gate_part * sig * up_part * gate
            return act.astype(LOW), jnp.concatenate([grad_gate.astype(LOW), grad_up.astype(LOW)])

        ups, downs = jnp.split(w_up, experts), jnp.split(w_down, experts)
        pairs = [both_ways(ups[e], downs[e], gates[e : e + 1]) for e in range(experts)]
        act_s, dgu_s = both_ways(s_up, s_down, 1.0)
        acts, dgus = (jnp.concatenate(parts) for parts in zip(*pairs))
        return hidden, grad, acts, act_s, dgus, dgu_s

    def rows_out(self, pairs, resid, gain, grad_rows):
        if self.line:
            return rows_out(self.line, pairs, resid, gain.reshape(1, -1), grad_rows, self.number())
        sums = []
        for pair in pairs:
            term = sum(dot_tn(left, right) for left, right in pair).astype(LOW)
            term = lax.psum_scatter(term, self.AXES["all"], scatter_dimension=0, tiled=True)
            sums.append(term.astype(jnp.float32))
        inv = lax.rsqrt(jnp.mean(resid * resid, axis=-1, keepdims=True) + EPS)
        grad_resid, grad_gain = rms_backward(resid, inv, gain, sums[0])
        grad_resid = grad_resid + grad_rows.astype(jnp.float32)
        grad_all = lax.all_gather(grad_resid.astype(LOW), "narrow", axis=0, tiled=True)
        return sums[1], grad_resid, grad_gain, grad_all


def rows_of(array, index, count):
    return lax.dynamic_slice_in_dim(array, index * count, count, 0)


def dot_nt(lhs, rhs):
    return lax.dot_general(lhs, rhs, (((1,), (1,)), ((), ())), preferred_element_type=jnp.float32)


def dot_tn(lhs, rhs):
    return lax.dot_general(lhs, rhs, (((0,), (0,)), ((), ())), preferred_element_type=jnp.float32)


def dot_nn(lhs, rhs):
    return jnp.dot(lhs, rhs, preferred_element_type=jnp.float32)


def per_device(
    links,
    tokens_in,
    seg_ids,
    routes,
    gate_vals,
    attn_gain,
    w_query,
    w_latent,
    latent_gain,
    w_expand,
    w_output,
    ffn_gain,
    w_shared_in,
    w_shared_out,
    w_expert_in,
    w_expert_out,
    grad_output,
):
    links.calls = 0
    low = LOW
    wide_count = lax.axis_size("wide")
    narrow_count = lax.axis_size("narrow")
    wide_at = lax.axis_index("wide")
    narrow_at = lax.axis_index("narrow")
    tok_rows, width = tokens_in.shape
    own_rows = tok_rows // narrow_count
    local_experts, _, _, hidden_local = w_expert_in.shape
    num_experts = local_experts * wide_count
    head_local = w_query.shape[1] // (DH + DR)

    def mine(array):
        return rows_of(array, narrow_at, own_rows)

    x_float = tokens_in.astype(jnp.float32)
    x_normed, _ = rms_forward(x_float, attn_gain)
    x_low = x_normed.astype(low)
    latent_part = rows_of(w_latent.T, narrow_at, w_latent.shape[1] // narrow_count)
    chosen = routes[:, :, None] == jnp.arange(num_experts, dtype=jnp.int32)
    gate_table = jnp.sum(jnp.where(chosen, gate_vals[:, :, None], 0.0), axis=1).T
    gate_table = gate_table.reshape(wide_count, local_experts, tok_rows)
    gate_table = jnp.pad(gate_table, ((0, 0), (0, -local_experts % 8), (0, 0))).reshape(-1, tok_rows)
    wq_all, wkva_all, wkvb_all, wo_all, shared_in, shared_out, gates, x_part = links.move(
        links.gather(w_query, "wide", 0, (1, 5 * w_query.shape[1] // 6)),
        links.grid(latent_part),
        links.gather(w_expand, "wide", 0, (1, 7 * w_expand.shape[1] // 8)),
        links.gather(w_output, "wide", 1, (0, 7 * w_output.shape[0] // 8)),
        links.swap(w_shared_in.transpose(1, 2, 0), "wswap", 1, 2),
        links.swap(w_shared_out, "wswap", 0, 1),
        links.swap(gate_table, "wswap", 0, 1),
        links.swap(mine(x_low), "wswap", 1, 0),
    )

    cos_tab, sin_tab = rotary_tables(positions(seg_ids))
    queries = dot_nn(x_low, wq_all).reshape(tok_rows, head_local, DH + DR).transpose(1, 0, 2)
    q_heads = jnp.concatenate(
        [queries[..., :DH], rotate(queries[..., DH:], cos_tab, sin_tab)], -1
    ).astype(low)
    latent_all = dot_nt(x_low, wkva_all)
    latent = latent_all[:, :KVR]
    latent_normed, _ = rms_forward(latent, latent_gain)
    latent_low = latent_normed.astype(low)
    key_rope = rotate(latent_all[:, KVR:], cos_tab, sin_tab).astype(low)
    expanded = dot_nn(latent_low, wkvb_all).reshape(tok_rows, head_local, 2 * DH).transpose(1, 0, 2)
    key_nope = expanded[..., :DH].astype(low)
    v_heads = expanded[..., DH:].astype(low)
    k_heads = jnp.concatenate(
        [key_nope, jnp.broadcast_to(key_rope[None], (head_local, tok_rows, DR))], -1
    )
    attended, log_total = attention_forward(q_heads, k_heads, v_heads, seg_ids)
    merged = attended.transpose(1, 0, 2).reshape(tok_rows, head_local * DH)
    mixed = links.narrow_sum(dot_nn(merged, wo_all).astype(low))

    x_rows = mine(x_float)
    resid = x_rows + mixed
    resid_normed, _ = rms_forward(resid, ffn_gain)

    expert_rows = local_experts * hidden_local
    w_up = w_expert_in.transpose(0, 2, 3, 1).reshape(2 * expert_rows, width)
    w_down = w_expert_out.reshape(expert_rows, width)
    s_up = shared_in.reshape(-1, width)
    hidden, grad_all, act_exp, act_sh, grad_gu_exp, grad_gu_sh = links.rows_in(
        resid_normed.astype(low), mine(grad_output), gates, w_up, s_up, w_down, shared_out, local_experts
    )
    out_rows, grad_resid, grad_ffn, grad_low = links.rows_out(
        (((grad_gu_exp, w_up), (grad_gu_sh, s_up)), ((act_exp, w_down), (act_sh, shared_out))),
        resid,
        ffn_gain,
        mine(grad_output),
    )
    grad_exp_out = dot_nn(act_exp, grad_all).reshape(local_experts, hidden_local, width)
    grad_shout = dot_nn(act_sh, grad_all).astype(low)
    grad_exp_in = dot_nn(grad_gu_exp, hidden).reshape(local_experts, 2, hidden_local, width)
    grad_exp_in = grad_exp_in.transpose(0, 3, 1, 2)
    grad_shin = dot_nn(grad_gu_sh, hidden).reshape(2, -1, width).astype(low)
    out_rows = (resid + out_rows).astype(low)

    grad_merged = dot_nt(grad_low, wo_all)
    grad_wo = dot_tn(merged, grad_low).astype(low)
    red_wo = lax.psum_scatter(grad_wo, "wide", scatter_dimension=1, tiled=True)
    grad_att = grad_merged.reshape(tok_rows, head_local, DH).transpose(1, 0, 2).astype(low)
    grad_q, grad_k, grad_v = attention_backward(
        q_heads, k_heads, v_heads, grad_att, log_total, seg_ids
    )
    grad_q_pre = jnp.concatenate(
        [grad_q[..., :DH], unrotate(grad_q[..., DH:], cos_tab, sin_tab)], -1
    ).astype(low)
    grad_q_pre = grad_q_pre.transpose(1, 0, 2).reshape(tok_rows, head_local * (DH + DR))
    grad_rope_part = jnp.sum(grad_k[..., DH:], axis=0)
    grad_expanded = jnp.concatenate([grad_k[..., :DH], grad_v], -1).astype(low)
    grad_expanded = grad_expanded.transpose(1, 0, 2).reshape(tok_rows, head_local * 2 * DH)
    grad_wkvb = dot_tn(latent_low, grad_expanded).astype(low)
    grad_latent_part = dot_nt(grad_expanded, wkvb_all)
    grad_x_part = dot_nt(grad_q_pre, wq_all)
    half = DR // 2
    rope_pad = jnp.zeros((tok_rows, 128 - DR), jnp.float32)
    changed = (grad_rope_part[:, half:], grad_rope_part[:, :half])
    terms = jnp.concatenate(
        [grad_x_part, grad_latent_part, grad_rope_part, rope_pad, *changed, rope_pad], 1
    ).astype(low)
    cos_rows, sin_rows = mine(cos_tab), mine(sin_tab)
    lane_pad = jnp.zeros((own_rows, 128 - DR), jnp.float32)
    cos_sin = jnp.stack([
        jnp.concatenate([cos_rows, cos_rows, lane_pad], 1),
        jnp.concatenate([sin_rows, -sin_rows, lane_pad], 1),
    ])
    (q_pre_all, red_wkvb, x_cols, layer_out, red_shout, red_shin, grad_tokens, latent_rows, rope_rows,
     gains) = links.move_back(
        (
            links.gather(grad_q_pre, "wide", 0, (1, 5 * grad_q_pre.shape[1] // 6)),
            links.wide_sum(grad_wkvb, 0),
            links.weave(x_part.reshape(wide_count, own_rows, -1)),
            links.swap(out_rows, "nswap", 1, 0),
            links.swap(grad_shout, "wswap", 1, 0),
            links.swap(grad_shin, "wswap", 2, 1),
        ),
        (
            terms,
            mine(latent),
            cos_sin,
            latent_gain.reshape(1, -1),
            wkva_all[:KVR],
            wkva_all[KVR:],
            mine(tokens_in),
            attn_gain.reshape(1, -1),
            grad_resid,
            grad_ffn.reshape(1, -1),
        ),
    )
    x_cols = x_cols.reshape(wide_count * tok_rows, -1)
    red_wkva = dot_tn(x_cols, jnp.concatenate([latent_rows, rope_rows[:, :DR]], 1))
    red_wq = dot_tn(x_cols, q_pre_all)
    gains = jnp.sum(gains, axis=(0, 1))
    part = width // wide_count
    lat_part = KVR // wide_count
    red_att_gain = rows_of(gains[:width], wide_at, part)
    red_ffn = rows_of(gains[width : 2 * width], wide_at, part)
    red_lat_gain = rows_of(gains[2 * width :], wide_at, lat_part)
    return (
        layer_out,
        grad_tokens.astype(jnp.float32),
        red_att_gain,
        red_wq,
        red_wkva,
        red_lat_gain,
        red_wkvb,
        red_wo.astype(jnp.float32),
        red_ffn,
        red_shin.astype(jnp.float32).transpose(2, 0, 1),
        red_shout.astype(jnp.float32),
        grad_exp_in,
        grad_exp_out,
    )


def solution(mesh):
    placed = (
        P("wide", None),
        P("wide"),
        P("wide", None),
        P("wide", None),
        P(),
        P("wide", "narrow"),
        P("wide", None),
        P(),
        P("wide", "narrow"),
        P("narrow", "wide"),
        P(),
        P("wide", None, "narrow"),
        P("narrow", "wide"),
        P("wide", None, None, "narrow"),
        P("wide", "narrow", None),
        P("wide", None),
    )
    return jax.shard_map(
        functools.partial(per_device, Links(mesh)),
        mesh=mesh,
        in_specs=placed,
        out_specs=(
            P("wide", "narrow"),
            P("wide", None),
            P("wide"),
            P("wide", "narrow"),
            P("wide", None),
            P("wide"),
            P("wide", "narrow"),
            P("narrow", "wide"),
            P("wide"),
            P("wide", None, "narrow"),
            P("narrow", "wide"),
            P("wide", None, None, "narrow"),
            P("wide", "narrow", None),
        ),
        check_vma=False,
    )
```
